512 devices in a mesh: groups: 2 (over y), space: 32 (over z), rhs: 8 (over x, core).
Axes of the slice: x: 4, y: 2, z: 32, core: 2. Of those that a mesh axis runs over, the one named last changes fastest.
The devices are a block of a 4x8x32 slice.
Arguments:
- conductance: float32 [512, 1024], P(('groups', 'space')), parts along dimension 0, may hold values from 0.05 to 2
- nodata: int32 [512, 1024], P(('groups', 'space')), parts along dimension 0, may hold values 0 or 1
- ground_mask: int32 [512, 1024], P(('groups', 'space')), parts along dimension 0, may hold values 0 or 1
- ground_value: float32 [512, 1024], P(('groups', 'space')), parts along dimension 0, may hold values from 0.5 to 4
- source_mask: int32 [512, 1024], P(('groups', 'space')), parts along dimension 0, may hold values 0 or 1
- source_current: float32 [512, 1024], P(('groups', 'space')), parts along dimension 0, may hold values from 0.5 to 4
- tile_inverse: float32 [512, 8, 128, 128], P(('groups', 'space')), parts along dimension 0, may hold values from -0.04 to 8, as said below
- focal_cells: int32 [1024, 2], P(('groups', 'rhs')), parts along dimension 0, may hold values from 0 to 262143
Outputs:
- solution: float32 [512, 512, 1024], P('rhs', ('groups', 'space')), parts along dimension 1
- residual: float32 [512, 512, 1024], P('rhs', ('groups', 'space')), parts along dimension 1
The draws below stay inside these ranges and needn't reach their ends.
There are 2 independent parts, one for each index of `groups`. The reference program is written for one: setup_inputs(seed, part) draws one part's arguments, and reference() takes and returns one part's arrays. A program takes and returns all parts, laid end to end along the dimension named above; each array names one. Nothing has to cross between parts.
Inputs may be any that keep to these rules, and one draw needn't show every extreme that they name: `tile_inverse`: each block is symmetric positive definite.
All inputs are finite; a program needn't handle non-finite values. No bound on the sum of `nodata` or of `ground_mask` or of `source_mask` on one device may be relied on, other than what follows from the above.
Results may differ from the reference program's by a relative error of at most 0.00025.
Values sent between devices are 32-bit elements; how exact they have to be, the bound alone decides.
No kernel may reach another device: no remote copies, remote signals or barrier semaphores. Data moves between devices by JAX's collectives and lax.ppermute only.
A program may use at most 64 MiB of HBM per device.

```python
import math
import jax
import jax.numpy as jnp
from jax import lax

NC = 1024
ITERS = 2
NR = 256
PAIRS = 512


def draw_tile_inverse(key, part):
    key_off, key_diag = jax.random.split(jax.random.fold_in(key, 7))
    block_shape = (NR, NC // 128, 128, 128)
    spread_top = 0.02
    lower_end = 0.5
    upper_end = 1.5
    raw_values = jax.random.uniform(key_off, block_shape, jnp.float32, -spread_top, spread_top)
    upper_half = jnp.triu(raw_values, 1)
    off_part = upper_half + jnp.swapaxes(upper_half, -1, -2)
    base_part = jax.random.uniform(key_diag, block_shape[:-1], jnp.float32, lower_end, upper_end)
    diag_part = jnp.sum(jnp.abs(off_part), axis=-1) + base_part
    return off_part + diag_part[..., None] * jnp.eye(128, dtype=jnp.float32)


def set_ends(values, rng, least, high):
    place = [jax.random.randint(jax.random.fold_in(rng, axis), (), 0, length) for axis, length in enumerate(values.shape)]
    main_axis = values.shape.index(max(values.shape))
    neighbour = place[:main_axis] + [(place[main_axis] + 1) % values.shape[main_axis]] + place[main_axis + 1:]
    return values.at[tuple(place)].set(least).at[tuple(neighbour)].set(high)


def shard_levels(key, shape, cuts, smallest, top_value):
    gain, own = 1.0, jax.random.fold_in(key, 6)
    for dim, blocks in cuts:
        heights = jnp.exp(jax.random.uniform(jax.random.fold_in(own, dim), (blocks,), jnp.float32, smallest / len(cuts), top_value / len(cuts)))
        gain = gain * jnp.repeat(heights, shape[dim] // blocks).reshape([-1 if axis == dim else 1 for axis in range(len(shape))])
    return gain


def setup_inputs(seed: int = 0, part: int = 0) -> dict:
    keys = jax.random.split(jax.random.key(seed), 9)
    part_keys = jax.random.split(jax.random.fold_in(keys[8], part), 9)
    return {
        "conductance": jnp.clip(jnp.exp(math.log(2.0) - 3.6888794 * jax.random.uniform(part_keys[0], (NR, NC), jnp.float32) ** shard_levels(part_keys[0], (NR, NC), ((0, 32),), -0.2, 0.2)), 0.05, 2.0),
        "nodata": set_ends((jax.random.randint(part_keys[1], (NR, NC), 0, 10) < 1).astype(jnp.int32), jax.random.fold_in(part_keys[1], 1), 0, 1),
        "ground_mask": set_ends((jax.random.randint(part_keys[2], (NR, NC), 0, 20) < 1).astype(jnp.int32), jax.random.fold_in(part_keys[2], 1), 0, 1),
        "ground_value": jnp.clip(jnp.exp(math.log(4.0) - 2.0794415 * jax.random.uniform(part_keys[3], (NR, NC), jnp.float32) ** shard_levels(part_keys[3], (NR, NC), ((0, 32),), -0.2, 0.2)), 0.5, 4.0),
        "source_mask": set_ends((jax.random.randint(part_keys[4], (NR, NC), 0, 3) < 1).astype(jnp.int32), jax.random.fold_in(part_keys[4], 1), 0, 1),
        "source_current": jnp.clip(jnp.exp(math.log(4.0) - 2.0794415 * jax.random.uniform(part_keys[5], (NR, NC), jnp.float32) ** shard_levels(part_keys[5], (NR, NC), ((0, 32),), -0.2, 0.2)), 0.5, 4.0),
        "tile_inverse": draw_tile_inverse(jax.random.fold_in(jax.random.fold_in(keys[8], part), 71), part),
        "focal_cells": set_ends(jax.random.randint(part_keys[7], (PAIRS, 2), 0, NR * NC), jax.random.fold_in(part_keys[7], 1), 0, (NR * NC) - 1).astype(jnp.int32),
    }


LEAKAGE = 0.05
FOCAL_CURRENT = 16.0


def weights_from(padded_g, padded_v, valid_mask, ground_mask, ground_value):
    centre = padded_g[1:-1, 1:-1]
    north_w = 0.5 * (centre + padded_g[:-2, 1:-1]) * valid_mask * padded_v[:-2, 1:-1]
    south_w = 0.5 * (centre + padded_g[2:, 1:-1]) * valid_mask * padded_v[2:, 1:-1]
    west_w = 0.5 * (centre + padded_g[1:-1, :-2]) * valid_mask * padded_v[1:-1, :-2]
    east_w = 0.5 * (centre + padded_g[1:-1, 2:]) * valid_mask * padded_v[1:-1, 2:]
    grounded = ground_mask.astype(jnp.float32) * ground_value
    diagonal = valid_mask * (LEAKAGE + grounded) + (1.0 - valid_mask) + north_w + south_w + west_w + east_w
    return diagonal, north_w, south_w, west_w, east_w


def stencil(padded, weights):
    diagonal, north_w, south_w, west_w, east_w = weights
    centre = padded[:, 1:-1, 1:-1]
    return (diagonal * centre - north_w * padded[:, :-2, 1:-1] - south_w * padded[:, 2:, 1:-1]
            - west_w * padded[:, 1:-1, :-2] - east_w * padded[:, 1:-1, 2:])


def precondition(field_in, tile_inverse):
    pair_count, row_count, col_count = field_in.shape
    blocks = field_in.reshape(pair_count, row_count, col_count // 128, 128)
    result = jnp.einsum("rcij,prcj->prci", tile_inverse, blocks,
                        precision=lax.Precision.HIGHEST, preferred_element_type=jnp.float32)
    return result.reshape(pair_count, row_count, col_count)


def inner_sum(first, second):
    return jnp.sum(first * second, axis=(1, 2))


def reference(conductance, nodata, ground_mask, ground_value, source_mask, source_current, tile_inverse, focal_cells):
    valid_mask = (1 - nodata).astype(jnp.float32)
    active = conductance * valid_mask
    weights = weights_from(jnp.pad(active, 1), jnp.pad(valid_mask, 1), valid_mask, ground_mask, ground_value)
    row_count, col_count = conductance.shape
    cell_ids = jnp.arange(row_count * col_count, dtype=jnp.int32)
    onehot = ((cell_ids[None, :] == focal_cells[:, 0:1]).astype(jnp.float32)
              - (cell_ids[None, :] == focal_cells[:, 1:2]).astype(jnp.float32))
    onehot = onehot.reshape(focal_cells.shape[0], row_count, col_count)
    background = source_mask.astype(jnp.float32) * source_current
    right_side = background[None] + FOCAL_CURRENT * onehot
    solution = jnp.zeros_like(right_side)
    residual = right_side
    precond = precondition(residual, tile_inverse)
    direction = precond
    gamma_now = inner_sum(residual, precond)
    for iteration in range(ITERS):
        padded = jnp.pad(direction, ((0, 0), (1, 1), (1, 1)))
        image = stencil(padded, weights)
        step_len = gamma_now / inner_sum(direction, image)
        solution = solution + step_len[:, None, None] * direction
        residual = residual - step_len[:, None, None] * image
        if iteration + 1 < ITERS:
            precond = precondition(residual, tile_inverse)
            gamma_next = inner_sum(residual, precond)
            direction = precond + (gamma_next / gamma_now)[:, None, None] * direction
            gamma_now = gamma_next
    return solution, residual
```

```python
import functools

import jax
import jax.numpy as jnp
from jax import lax
from jax.experimental import pallas as pl
from jax.experimental.pallas import tpu as pltpu
from jax.sharding import PartitionSpec as P

LEAKAGE = 0.05
FOCAL_CURRENT = 16.0
TILE = 128
CHUNK = 16
MIB = 1024 * 1024


def cut(x):
    high = x.astype(jnp.bfloat16)
    return high, (x - high.astype(jnp.float32)).astype(jnp.bfloat16)


def load(field, at):
    return jnp.concatenate([field[t, at, :] for t in range(field.shape[0])], axis=1)


def store(field, at, x):
    for t in range(field.shape[0]):
        field[t, at, :] = x[:, t * TILE : (t + 1) * TILE]


def apply_tiles(src, dst, tiles, row, rows, count):
    chunks = (count + CHUNK - 1) // CHUNK

    for t in range(src.shape[0]):
        high, low = cut(tiles[0, t])

        def one(c, _):
            at = pl.ds(c * (CHUNK * rows) + row, CHUNK, stride=rows)
            x_high, x_low = cut(src.at[t][at, :])
            x = jnp.concatenate([x_high, x_low], axis=0)
            a = jnp.dot(x, high, preferred_element_type=jnp.float32)
            b = jnp.dot(x, low, preferred_element_type=jnp.float32)
            dst.at[t][at, :] = (a[:CHUNK] + b[CHUNK:]) + (a[CHUNK:] + b[:CHUNK])
            return 0

        one(0, 0)
        lax.fori_loop(1, chunks, one, 0)


def shifted(x, above, below, rows, cols):
    row = lax.broadcasted_iota(jnp.int32, (rows, cols), 0)
    up = jnp.where(row == 0, above, pltpu.roll(x, 1, 0))
    down = jnp.where(row == rows - 1, below, pltpu.roll(x, rows - 1, 0))
    return up, down, pltpu.roll(x, 1, 1), pltpu.roll(x, cols - 1, 1)


def operator(x, above, below, weights, rows, cols):
    up, down, left, right = shifted(x, above, below, rows, cols)
    diag, north, south, west, east = weights
    return diag * x - north * up - south * down - west * left - east * right


def fill_rims(field, index, up_ref, down_ref, rows, pairs, count):
    cols = up_ref.shape[1]
    first, last = load(field, slice(0, 1)), load(field, slice(rows - 1, rows))
    up_ref[0 : pairs + 8, :] = jnp.broadcast_to(first, (pairs + 8, cols))
    down_ref[0 : pairs + 8, :] = jnp.broadcast_to(last, (pairs + 8, cols))

    def one(s, _):
        k = index[pairs + s]
        up_ref[pl.ds(k, 1), :] = load(field, pl.ds(s * rows, 1))
        down_ref[pl.ds(k, 1), :] = load(field, pl.ds(s * rows + rows - 1, 1))
        return 0

    lax.fori_loop(1, count, one, 0)


def start_kernel(
    where, focal, mask, current, cond, nodata, tiles, field, pre, index, up_ref, down_ref, *, rows, cols, pairs, slots
):
    r = pl.program_id(0)
    base_row = where[0]

    @pl.when(r == 0)
    def _():
        background = mask[...].astype(jnp.float32) * current[...]
        store(field, slice(0, rows), background)
        index[pairs] = pairs

        def listed(k, s):
            a = lax.div(focal[2 * k], cols) - base_row
            b = lax.div(focal[2 * k + 1], cols) - base_row
            near = ((a >= -2) & (a < rows + 2)) | ((b >= -2) & (b < rows + 2))
            index[k] = jnp.where(near, s, 0)

            @pl.when(near)
            def _():
                index[pairs + s] = k

            return s + near.astype(jnp.int32)

        count = lax.fori_loop(0, pairs, listed, jnp.int32(1))
        index[pairs + slots] = count
        lane = lax.broadcasted_iota(jnp.int32, (1, TILE), 1)

        def one(s, _):
            k = index[pairs + s]
            store(field, pl.ds(s * rows, rows), background)
            for end in range(2):
                cell = focal[2 * k + end]
                i = lax.div(cell, cols)
                j = cell - i * cols
                i = i - base_row

                @pl.when((i >= 0) & (i < rows))
                def _():
                    t = lax.div(j, TILE)
                    at = pl.ds(s * rows + i, 1)
                    sign = FOCAL_CURRENT * (1 - 2 * end)
                    field[t, at, :] = field[t, at, :] + jnp.where(lane == j - t * TILE, sign, 0.0)

            return 0

        lax.fori_loop(1, count, one, 0)

    count = index[pairs + slots]
    apply_tiles(field, pre, tiles, r, rows, count)

    @pl.when(r == rows - 1)
    def _():
        fill_rims(pre, index, up_ref, down_ref, rows, pairs, count)
        valid = (1 - nodata[...]).astype(jnp.float32)
        active = cond[...] * valid
        up_ref[pairs + 1 : pairs + 2, :] = active[0:1, :]
        up_ref[pairs + 2 : pairs + 3, :] = valid[0:1, :]
        down_ref[pairs + 1 : pairs + 2, :] = active[rows - 1 : rows, :]
        down_ref[pairs + 2 : pairs + 3, :] = valid[rows - 1 : rows, :]


def middle_kernel(
    index,
    cond,
    nodata,
    ground_mask,
    ground_value,
    pre,
    above,
    below,
    tiles,
    image,
    second,
    weights,
    up_ref,
    down_ref,
    *,
    rows,
    cols,
    pairs,
    slots,
):
    r = pl.program_id(0)
    count = index[pairs + slots]

    @pl.when(r == 0)
    def _():
        valid = (1 - nodata[...]).astype(jnp.float32)
        active = cond[...] * valid
        lane = lax.broadcasted_iota(jnp.int32, (rows, cols), 1)
        g = shifted(active, above[pairs + 1 : pairs + 2, :], below[pairs + 1 : pairs + 2, :], rows, cols)
        v = shifted(valid, above[pairs + 2 : pairs + 3, :], below[pairs + 2 : pairs + 3, :], rows, cols)
        inside = (None, None, lane > 0, lane < cols - 1)
        edges = []
        for n in range(4):
            edge = 0.5 * (active + g[n]) * valid * v[n]
            if inside[n] is not None:
                edge = jnp.where(inside[n], edge, 0.0)
            edges.append(edge)
        grounded = ground_mask[...].astype(jnp.float32) * ground_value[...]
        diag = valid * (LEAKAGE + grounded) + (1.0 - valid) + edges[0] + edges[1] + edges[2] + edges[3]
        for n, x in enumerate([diag, *edges]):
            weights[n * rows : (n + 1) * rows, :] = x

        def one(s, _):
            k = index[pairs + s]
            at = pl.ds(s * rows, rows)
            w = [weights[n * rows : (n + 1) * rows, :] for n in range(5)]
            store(image, at, operator(load(pre, at), above[pl.ds(k, 1), :], below[pl.ds(k, 1), :], w, rows, cols))
            return 0

        lax.fori_loop(0, count, one, 0)

    apply_tiles(image, second, tiles, r, rows, count)

    @pl.when(r == rows - 1)
    def _():
        fill_rims(second, index, up_ref, down_ref, rows, pairs, count)


def sums_kernel(
    index, field, pre, image, second, above, below, weights, last, sums, one_two, three_four, *, rows, cols, pairs, slots
):
    count = index[pairs + slots]

    def folded(x):
        acc = x[:, 0:TILE]
        for t in range(1, cols // TILE):
            acc = acc + x[:, t * TILE : (t + 1) * TILE]
        return jnp.sum(acc, axis=0, keepdims=True)

    def four(s):
        k = index[pairs + s]
        at = pl.ds(s * rows, rows)
        w = [weights[n * rows : (n + 1) * rows, :] for n in range(5)]
        u = load(second, at)
        v = operator(u, above[pl.ds(k, 1), :], below[pl.ds(k, 1), :], w, rows, cols)
        store(last, at, v)
        z, i = load(pre, at), load(image, at)
        return k, folded(load(field, at) * z), folded(z * i), folded(i * u), folded(u * v)

    _, a, b, c, d = four(0)
    one_two[0:pairs, :] = jnp.broadcast_to(a, (pairs, TILE))
    one_two[pairs : 2 * pairs, :] = jnp.broadcast_to(b, (pairs, TILE))
    three_four[0:pairs, :] = jnp.broadcast_to(c, (pairs, TILE))
    three_four[pairs : 2 * pairs, :] = jnp.broadcast_to(d, (pairs, TILE))

    def one(s, _):
        k, a, b, c, d = four(s)
        one_two[pl.ds(k, 1), :] = a
        one_two[pl.ds(pairs + k, 1), :] = b
        three_four[pl.ds(k, 1), :] = c
        three_four[pl.ds(pairs + k, 1), :] = d
        return 0

    lax.fori_loop(1, count, one, 0)
    sums[0:1, :] = jnp.sum(one_two[...].T, axis=0, keepdims=True)
    sums[1:2, :] = jnp.sum(three_four[...].T, axis=0, keepdims=True)


def finish_kernel(
    index, everyone, field, pre, image, second, last, solution, residual, first_c, second_c, *, rows, cols, pairs, block
):
    step = pl.program_id(0)

    @pl.when(step == 0)
    def _():
        total = jnp.sum(everyone[...], axis=0)
        ab, cd = total[0:1, :], total[1:2, :]
        gamma, delta = ab[:, :pairs], ab[:, pairs:]
        eta, theta = cd[:, :pairs], cd[:, pairs:]
        alpha = gamma / delta
        gamma_next = alpha * alpha * eta - gamma
        beta = 1.0 + gamma_next / gamma
        curvature = beta * beta * delta - 2.0 * beta * alpha * eta + alpha * alpha * theta
        step_next = gamma_next / curvature
        both = jnp.concatenate([alpha + step_next * beta, alpha * step_next], axis=1)
        spread = jnp.broadcast_to(both, (2 * pairs, 2 * pairs)).T
        first_c[...] = spread[:pairs, :]
        second_c[...] = spread[pairs:, :]

    def one(p, _):
        k = step * block + p
        s = index[k]
        at = pl.ds(s * rows, rows)
        a = jnp.broadcast_to(first_c[pl.ds(k, 1), :], (rows, TILE))
        b = jnp.broadcast_to(second_c[pl.ds(k, 1), :], (rows, TILE))
        for t in range(cols // TILE):
            lanes = slice(t * TILE, (t + 1) * TILE)
            solution[p, :, lanes] = a * pre[t, at, :] - b * second[t, at, :]
            residual[p, :, lanes] = field[t, at, :] - a * image[t, at, :] + b * last[t, at, :]
        return 0

    lax.fori_loop(0, block, one, 0, unroll=2)


def smem():
    return pl.BlockSpec(memory_space=pltpu.SMEM)


def whole(*shape):
    return pl.BlockSpec(shape, lambda *_: (0,) * len(shape))


def neighbours(up, down):
    count = lax.axis_size("space")
    ends = count - 1
    above = lax.ppermute(down, "space", [(i, (i + 1) % count) for i in range(ends)])
    below = lax.ppermute(up, "space", [((i + 1) % count, i) for i in range(ends)])
    return above, below


def on_device(conductance, nodata, ground_mask, ground_value, source_mask, source_current, tile_inverse, focal_cells):
    rows, cols = conductance.shape
    pairs = focal_cells.shape[0]
    slots = -(-(pairs + 1) // CHUNK) * CHUNK
    devices = lax.axis_size("space")
    f32 = jnp.float32
    sizes = dict(rows=rows, cols=cols, pairs=pairs, slots=slots)
    strip, fields, rim = (rows, cols), (cols // TILE, slots * rows, TILE), (pairs + 8, cols)
    tile_block = pl.BlockSpec((1, cols // TILE, TILE, TILE), lambda r: (r, 0, 0, 0))
    limit = pltpu.CompilerParams(vmem_limit_bytes=32 * MIB)
    base_row = (lax.axis_index("space") * rows).astype(jnp.int32).reshape(1)

    field, pre, index, up, down = pl.pallas_call(
        functools.partial(start_kernel, **sizes),
        grid=(rows,),
        in_specs=[smem(), smem(), whole(*strip), whole(*strip), whole(*strip), whole(*strip), tile_block],
        out_specs=[whole(*fields), whole(*fields), smem(), whole(*rim), whole(*rim)],
        out_shape=[
            jax.ShapeDtypeStruct(fields, f32),
            jax.ShapeDtypeStruct(fields, f32),
            jax.ShapeDtypeStruct((pairs + slots + 8,), jnp.int32),
            jax.ShapeDtypeStruct(rim, f32),
            jax.ShapeDtypeStruct(rim, f32),
        ],
        compiler_params=limit,
        name="start",
    )(base_row, focal_cells.reshape(-1), source_mask, source_current, conductance, nodata, tile_inverse)
    above, below = neighbours(up, down)

    image, second, weights, up, down = pl.pallas_call(
        functools.partial(middle_kernel, **sizes),
        grid=(rows,),
        in_specs=[smem(), *[whole(*strip)] * 4, whole(*fields), whole(*rim), whole(*rim), tile_block],
        out_specs=[whole(*fields), whole(*fields), whole(5 * rows, cols), whole(*rim), whole(*rim)],
        out_shape=[
            jax.ShapeDtypeStruct(fields, f32),
            jax.ShapeDtypeStruct(fields, f32),
            jax.ShapeDtypeStruct((5 * rows, cols), f32),
            jax.ShapeDtypeStruct(rim, f32),
            jax.ShapeDtypeStruct(rim, f32),
        ],
        compiler_params=limit,
        name="middle",
    )(index, conductance, nodata, ground_mask, ground_value, pre, above, below, tile_inverse)
    above, below = neighbours(up, down)

    last, sums = pl.pallas_call(
        functools.partial(sums_kernel, **sizes),
        grid=(1,),
        in_specs=[smem(), *[whole(*fields)] * 4, whole(*rim), whole(*rim), whole(5 * rows, cols)],
        out_specs=[whole(*fields), whole(2, 2 * pairs)],
        out_shape=[jax.ShapeDtypeStruct(fields, f32), jax.ShapeDtypeStruct((2, 2 * pairs), f32)],
        scratch_shapes=[pltpu.VMEM((2 * pairs, TILE), f32), pltpu.VMEM((2 * pairs, TILE), f32)],
        compiler_params=limit,
        name="sums",
    )(index, field, pre, image, second, above, below, weights)
    copies = jnp.broadcast_to(sums, (devices, *sums.shape))
    everyone = lax.all_to_all(copies, "space", split_axis=0, concat_axis=0, tiled=True)

    block = 8
    out = jax.ShapeDtypeStruct((pairs, rows, cols), f32)
    out_block = pl.BlockSpec((block, rows, cols), lambda p: (p, 0, 0))
    return pl.pallas_call(
        functools.partial(finish_kernel, rows=rows, cols=cols, pairs=pairs, block=block),
        grid=(pairs // block,),
        in_specs=[smem(), whole(devices, 2, 2 * pairs), *[whole(*fields)] * 5],
        out_specs=[out_block, out_block],
        out_shape=[out, out],
        scratch_shapes=[pltpu.VMEM((pairs, TILE), f32), pltpu.VMEM((pairs, TILE), f32)],
        compiler_params=limit,
        name="finish",
    )(index, everyone, field, pre, image, second, last)


def solution(mesh):
    cells = P(("groups", "space"), None)
    return jax.shard_map(
        on_device,
        mesh=mesh,
        in_specs=(*[cells] * 6, P(("groups", "space"), None, None, None), P(("groups", "rhs"), None)),
        out_specs=(P("rhs", ("groups", "space"), None), P("rhs", ("groups", "space"), None)),
        check_vma=False,
    )
```

```python
import functools

import jax
import jax.numpy as jnp
from jax import lax
from jax.experimental import pallas as pl
from jax.experimental.pallas import tpu as pltpu
from jax.sharding import PartitionSpec as P

LEAKAGE = 0.05
FOCAL_CURRENT = 16.0
TILE = 128
CHUNK = 16
MIB = 1024 * 1024


def cut(x):
    high = x.astype(jnp.bfloat16)
    return high, (x - high.astype(jnp.float32)).astype(jnp.bfloat16)


def load(field, at):
    return jnp.concatenate([field[t, at, :] for t in range(field.shape[0])], axis=1)


def store(field, at, x):
    for t in range(field.shape[0]):
        field[t, at, :] = x[:, t * TILE : (t + 1) * TILE]


def times_tile(x, pair):
    x_high, x_low = cut(x)
    y = jnp.dot(jnp.concatenate([x_high, x_low], axis=0), pair, preferred_element_type=jnp.float32)
    n = x.shape[0]
    return (y[:n, :TILE] + y[n:, TILE:]) + (y[n:, :TILE] + y[:n, TILE:])


def apply_tiles(src, dst, parts, rows, chunks, first):
    def one(i, _):
        c = lax.div(i, rows)
        r = i - c * rows
        at = pl.ds(c * (CHUNK * rows) + r, CHUNK, stride=rows)
        for t in range(src.shape[0]):
            dst.at[t][at, :] = times_tile(src.at[t][at, :], parts[r, t])
        return 0

    lax.fori_loop(first * rows, chunks * rows, one, 0)


def shifted(x, above, below, rows, cols):
    row = lax.broadcasted_iota(jnp.int32, (rows, cols), 0)
    up = jnp.where(row == 0, above, pltpu.roll(x, 1, 0))
    down = jnp.where(row == rows - 1, below, pltpu.roll(x, rows - 1, 0))
    return up, down, pltpu.roll(x, 1, 1), pltpu.roll(x, cols - 1, 1)


def operator(x, above, below, weights, rows, cols):
    up, down, left, right = shifted(x, above, below, rows, cols)
    diag, north, south, west, east = weights
    return diag * x - north * up - south * down - west * left - east * right


def fill_rims(field, index, up_ref, down_ref, rows, pairs, count):
    cols = up_ref.shape[1]
    first, last = load(field, slice(0, 1)), load(field, slice(rows - 1, rows))
    up_ref[0 : pairs + 8, :] = jnp.broadcast_to(first, (pairs + 8, cols))
    down_ref[0 : pairs + 8, :] = jnp.broadcast_to(last, (pairs + 8, cols))

    def one(s, _):
        k = index[pairs + s]
        up_ref[pl.ds(k, 1), :] = load(field, pl.ds(s * rows, 1))
        down_ref[pl.ds(k, 1), :] = load(field, pl.ds(s * rows + rows - 1, 1))
        return 0

    lax.fori_loop(1, count, one, 0)


def start_kernel(
    where,
    focal_hbm,
    mask_hbm,
    current_hbm,
    cond_hbm,
    nodata_hbm,
    ground_mask_hbm,
    ground_value_hbm,
    tiles_hbm,
    field,
    pre,
    index,
    parts,
    cells,
    up_ref,
    down_ref,
    focal,
    mask,
    current,
    cond,
    nodata,
    ground_mask,
    ground_value,
    tiles,
    focal_sem,
    small_sems,
    tile_sems,
    *,
    rows,
    cols,
    pairs,
    slots,
):
    cells_of_pairs = pltpu.make_async_copy(focal_hbm, focal, focal_sem)
    cells_of_pairs.start()
    arrivals = [
        pltpu.make_async_copy(src, dst, small_sems.at[n])
        for n, (src, dst) in enumerate(
            [
                (mask_hbm, mask),
                (current_hbm, current),
                (cond_hbm, cond),
                (nodata_hbm, nodata),
                (ground_mask_hbm, ground_mask),
                (ground_value_hbm, ground_value),
            ]
        )
    ]
    for copy in arrivals:
        copy.start()
    for r in range(rows):
        pltpu.make_async_copy(tiles_hbm.at[r], tiles.at[r], tile_sems.at[r]).start()

    base_row = where[0]
    index[pairs] = pairs
    cells_of_pairs.wait()

    def listed(k, s):
        a = lax.div(focal[0, k], cols) - base_row
        b = lax.div(focal[1, k], cols) - base_row
        near = ((a >= -2) & (a < rows + 2)) | ((b >= -2) & (b < rows + 2))
        index[k] = jnp.where(near, s, 0)

        @pl.when(near)
        def _():
            index[pairs + s] = k

        return s + near.astype(jnp.int32)

    count = lax.fori_loop(0, pairs, listed, jnp.int32(1))
    index[pairs + slots] = count
    chunks = (count + CHUNK - 1) // CHUNK

    for copy in arrivals:
        copy.wait()
    background = mask[...].astype(jnp.float32) * current[...]
    store(field, slice(0, rows), background)
    lane = lax.broadcasted_iota(jnp.int32, (1, TILE), 1)

    def one(s, _):
        k = index[pairs + s]
        store(field, pl.ds(s * rows, rows), background)
        for end in range(2):
            cell = focal[end, k]
            i = lax.div(cell, cols)
            j = cell - i * cols
            i = i - base_row

            @pl.when((i >= 0) & (i < rows))
            def _():
                t = lax.div(j, TILE)
                at = pl.ds(s * rows + i, 1)
                sign = FOCAL_CURRENT * (1 - 2 * end)
                field[t, at, :] = field[t, at, :] + jnp.where(lane == j - t * TILE, sign, 0.0)

        return 0

    lax.fori_loop(1, count, one, 0)

    valid = (1 - nodata[...]).astype(jnp.float32)
    active = cond[...] * valid
    cells[0:rows, :] = active
    cells[rows : 2 * rows, :] = valid
    cells[2 * rows : 3 * rows, :] = ground_mask[...].astype(jnp.float32) * ground_value[...]

    def row(r, _):
        pltpu.make_async_copy(tiles_hbm.at[r], tiles.at[r], tile_sems.at[r]).wait()
        at = pl.ds(r, CHUNK, stride=rows)
        for t in range(cols // TILE):
            pair = jnp.concatenate(cut(tiles[r, t]), axis=1)
            parts[r, t] = pair
            pre.at[t][at, :] = times_tile(field.at[t][at, :], pair)
        return 0

    lax.fori_loop(0, rows, row, 0)
    apply_tiles(field, pre, parts, rows, chunks, 1)

    fill_rims(pre, index, up_ref, down_ref, rows, pairs, count)
    up_ref[pairs + 1 : pairs + 2, :] = active[0:1, :]
    up_ref[pairs + 2 : pairs + 3, :] = valid[0:1, :]
    down_ref[pairs + 1 : pairs + 2, :] = active[rows - 1 : rows, :]
    down_ref[pairs + 2 : pairs + 3, :] = valid[rows - 1 : rows, :]


def middle_kernel(
    index, cells, pre, parts, above, below, image, second, weights, up_ref, down_ref, *, rows, cols, pairs, slots
):
    count = index[pairs + slots]
    active, valid, grounded = (cells[n * rows : (n + 1) * rows, :] for n in range(3))
    lane = lax.broadcasted_iota(jnp.int32, (rows, cols), 1)
    g = shifted(active, above[pairs + 1 : pairs + 2, :], below[pairs + 1 : pairs + 2, :], rows, cols)
    v = shifted(valid, above[pairs + 2 : pairs + 3, :], below[pairs + 2 : pairs + 3, :], rows, cols)
    inside = (None, None, lane > 0, lane < cols - 1)
    edges = []
    for n in range(4):
        edge = 0.5 * (active + g[n]) * valid * v[n]
        if inside[n] is not None:
            edge = jnp.where(inside[n], edge, 0.0)
        edges.append(edge)
    diag = valid * (LEAKAGE + grounded) + (1.0 - valid) + edges[0] + edges[1] + edges[2] + edges[3]
    for n, x in enumerate([diag, *edges]):
        weights[n * rows : (n + 1) * rows, :] = x

    def one(s, _):
        k = index[pairs + s]
        at = pl.ds(s * rows, rows)
        w = [weights[n * rows : (n + 1) * rows, :] for n in range(5)]
        store(image, at, operator(load(pre, at), above[pl.ds(k, 1), :], below[pl.ds(k, 1), :], w, rows, cols))
        return 0

    lax.fori_loop(0, count, one, 0)
    apply_tiles(image, second, parts, rows, (count + CHUNK - 1) // CHUNK, 0)
    fill_rims(second, index, up_ref, down_ref, rows, pairs, count)


def sums_kernel(
    index, field, pre, image, second, above, below, weights, last, sums, one_two, three_four, *, rows, cols, pairs, slots
):
    count = index[pairs + slots]

    def folded(x):
        acc = x[:, 0:TILE]
        for t in range(1, cols // TILE):
            acc = acc + x[:, t * TILE : (t + 1) * TILE]
        return jnp.sum(acc, axis=0, keepdims=True)

    def four(s):
        k = index[pairs + s]
        at = pl.ds(s * rows, rows)
        w = [weights[n * rows : (n + 1) * rows, :] for n in range(5)]
        u = load(second, at)
        v = operator(u, above[pl.ds(k, 1), :], below[pl.ds(k, 1), :], w, rows, cols)
        store(last, at, v)
        z, i = load(pre, at), load(image, at)
        return k, folded(load(field, at) * z), folded(z * i), folded(i * u), folded(u * v)

    _, a, b, c, d = four(0)
    one_two[0:pairs, :] = jnp.broadcast_to(a, (pairs, TILE))
    one_two[pairs : 2 * pairs, :] = jnp.broadcast_to(b, (pairs, TILE))
    three_four[0:pairs, :] = jnp.broadcast_to(c, (pairs, TILE))
    three_four[pairs : 2 * pairs, :] = jnp.broadcast_to(d, (pairs, TILE))

    def one(s, _):
        k, a, b, c, d = four(s)
        one_two[pl.ds(k, 1), :] = a
        one_two[pl.ds(pairs + k, 1), :] = b
        three_four[pl.ds(k, 1), :] = c
        three_four[pl.ds(pairs + k, 1), :] = d
        return 0

    lax.fori_loop(1, count, one, 0)
    sums[0:1, :] = jnp.sum(one_two[...].T, axis=0, keepdims=True)
    sums[1:2, :] = jnp.sum(three_four[...].T, axis=0, keepdims=True)


def finish_kernel(
    index, everyone, field, pre, image, second, last, solution, residual, first_c, second_c, *, rows, cols, pairs, block
):
    step = pl.program_id(0)

    @pl.when(step == 0)
    def _():
        total = jnp.sum(everyone[...], axis=0)
        ab, cd = total[0:1, :], total[1:2, :]
        gamma, delta = ab[:, :pairs], ab[:, pairs:]
        eta, theta = cd[:, :pairs], cd[:, pairs:]
        alpha = gamma / delta
        gamma_next = alpha * alpha * eta - gamma
        beta = 1.0 + gamma_next / gamma
        curvature = beta * beta * delta - 2.0 * beta * alpha * eta + alpha * alpha * theta
        step_next = gamma_next / curvature
        both = jnp.concatenate([alpha + step_next * beta, alpha * step_next], axis=1)
        spread = jnp.broadcast_to(both, (2 * pairs, 2 * pairs)).T
        first_c[...] = spread[:pairs, :]
        second_c[...] = spread[pairs:, :]

    def one(p, _):
        k = step * block + p
        s = index[k]
        at = pl.ds(s * rows, rows)
        a = jnp.broadcast_to(first_c[pl.ds(k, 1), :], (rows, TILE))
        b = jnp.broadcast_to(second_c[pl.ds(k, 1), :], (rows, TILE))
        for t in range(cols // TILE):
            lanes = slice(t * TILE, (t + 1) * TILE)
            solution[p, :, lanes] = a * pre[t, at, :] - b * second[t, at, :]
            residual[p, :, lanes] = field[t, at, :] - a * image[t, at, :] + b * last[t, at, :]
        return 0

    lax.fori_loop(0, block, one, 0, unroll=4)


def smem():
    return pl.BlockSpec(memory_space=pltpu.SMEM)


def vmem():
    return pl.BlockSpec(memory_space=pltpu.VMEM)


def hbm():
    return pl.BlockSpec(memory_space=pltpu.HBM)


def neighbours(up, down):
    count = lax.axis_size("space")
    ends = count - 1
    above = lax.ppermute(down, "space", [(i, (i + 1) % count) for i in range(ends)])
    below = lax.ppermute(up, "space", [((i + 1) % count, i) for i in range(ends)])
    return above, below


def on_device(conductance, nodata, ground_mask, ground_value, source_mask, source_current, tile_inverse, focal_cells):
    rows, cols = conductance.shape
    pairs = focal_cells.shape[0]
    slots = -(-(pairs + 1) // CHUNK) * CHUNK
    devices = lax.axis_size("space")
    f32 = jnp.float32
    sizes = dict(rows=rows, cols=cols, pairs=pairs, slots=slots)
    strip, fields, rim = (rows, cols), (cols // TILE, slots * rows, TILE), (pairs + 8, cols)
    per_row = tile_inverse.shape[1:]
    limit = pltpu.CompilerParams(vmem_limit_bytes=24 * MIB)
    base_row = (lax.axis_index("space") * rows).astype(jnp.int32).reshape(1)

    def shaped(shape, dtype=f32):
        return jax.ShapeDtypeStruct(shape, dtype)

    field, pre, index, parts, cells, up, down = pl.pallas_call(
        functools.partial(start_kernel, **sizes),
        in_specs=[smem(), *[hbm()] * 8],
        out_specs=[vmem(), vmem(), smem(), *[vmem()] * 4],
        out_shape=[
            shaped(fields),
            shaped(fields),
            shaped((pairs + slots + 8,), jnp.int32),
            shaped((rows, *per_row[:2], 2 * TILE), jnp.bfloat16),
            shaped((3 * rows, cols)),
            shaped(rim),
            shaped(rim),
        ],
        scratch_shapes=[
            pltpu.SMEM(focal_cells.shape[::-1], jnp.int32),
            pltpu.VMEM(strip, jnp.int32),
            pltpu.VMEM(strip, f32),
            pltpu.VMEM(strip, f32),
            pltpu.VMEM(strip, jnp.int32),
            pltpu.VMEM(strip, jnp.int32),
            pltpu.VMEM(strip, f32),
            pltpu.VMEM((rows, *per_row), f32),
            pltpu.SemaphoreType.DMA,
            pltpu.SemaphoreType.DMA((6,)),
            pltpu.SemaphoreType.DMA((rows,)),
        ],
        compiler_params=limit,
        name="start",
    )(
        base_row,
        *(
            pltpu.with_memory_space_constraint(x, pltpu.HBM)
            for x in (
                focal_cells.T,
                source_mask,
                source_current,
                conductance,
                nodata,
                ground_mask,
                ground_value,
                tile_inverse,
            )
        ),
    )
    above, below = neighbours(up, down)

    image, second, weights, up, down = pl.pallas_call(
        functools.partial(middle_kernel, **sizes),
        in_specs=[smem(), *[vmem()] * 5],
        out_specs=[vmem()] * 5,
        out_shape=[shaped(fields), shaped(fields), shaped((5 * rows, cols)), shaped(rim), shaped(rim)],
        compiler_params=limit,
        name="middle",
    )(index, cells, pre, parts, above, below)
    above, below = neighbours(up, down)

    last, sums = pl.pallas_call(
        functools.partial(sums_kernel, **sizes),
        in_specs=[smem(), *[vmem()] * 7],
        out_specs=[vmem()] * 2,
        out_shape=[shaped(fields), shaped((2, 2 * pairs))],
        scratch_shapes=[pltpu.VMEM((2 * pairs, TILE), f32), pltpu.VMEM((2 * pairs, TILE), f32)],
        compiler_params=limit,
        name="sums",
    )(index, field, pre, image, second, above, below, weights)
    copies = jnp.broadcast_to(sums, (devices, *sums.shape))
    everyone = lax.all_to_all(copies, "space", split_axis=0, concat_axis=0, tiled=True)

    block = 8
    out = jax.ShapeDtypeStruct((pairs, rows, cols), f32)
    out_block = pl.BlockSpec((block, rows, cols), lambda p: (p, 0, 0))
    return pl.pallas_call(
        functools.partial(finish_kernel, rows=rows, cols=cols, pairs=pairs, block=block),
        grid=(pairs // block,),
        in_specs=[smem(), *[vmem()] * 6],
        out_specs=[out_block, out_block],
        out_shape=[out, out],
        scratch_shapes=[pltpu.VMEM((pairs, TILE), f32), pltpu.VMEM((pairs, TILE), f32)],
        compiler_params=limit,
        name="finish",
    )(index, everyone, field, pre, image, second, last)


def solution(mesh):
    cells = P(("groups", "space"), None)
    return jax.shard_map(
        on_device,
        mesh=mesh,
        in_specs=(*[cells] * 6, P(("groups", "space"), None, None, None), P(("groups", "rhs"), None)),
        out_specs=(P("rhs", ("groups", "space"), None), P("rhs", ("groups", "space"), None)),
        check_vma=False,
    )
```

```python
import functools

import jax
import jax.numpy as jnp
from jax import lax
from jax.experimental import pallas as pl
from jax.experimental.pallas import tpu as pltpu
from jax.sharding import PartitionSpec as P

LEAKAGE = 0.05
FOCAL_CURRENT = 16.0
TILE = 128
CHUNK = 16
MIB = 1024 * 1024

RIM = 8


def cut(x):
    high = x.astype(jnp.bfloat16)
    return high, (x - high.astype(jnp.float32)).astype(jnp.bfloat16)


def load(field, at):
    return jnp.concatenate([field[t, at, :] for t in range(field.shape[0])], axis=1)


def store(field, at, x):
    for t in range(field.shape[0]):
        field[t, at, :] = x[:, t * TILE : (t + 1) * TILE]


def times_tile(x, pair):
    x_high, x_low = cut(x)
    y = jnp.dot(jnp.concatenate([x_high, x_low], axis=0), pair, preferred_element_type=jnp.float32)
    n = x.shape[0]
    return (y[:n, :TILE] + y[n:, TILE:]) + (y[n:, :TILE] + y[:n, TILE:])


def apply_tiles(src, dst, parts, rows, chunks, first):
    def one(i, _):
        c = lax.div(i, rows)
        r = i - c * rows
        at = pl.ds(c * (CHUNK * rows) + r, CHUNK, stride=rows)
        for t in range(src.shape[0]):
            dst.at[t][at, :] = times_tile(src.at[t][at, :], parts[r, t])
        return 0

    lax.fori_loop(first * rows, chunks * rows, one, 0)


def beside(x):
    cols = x.shape[1]
    return pltpu.roll(x, 1, 1), pltpu.roll(x, cols - 1, 1)


def stacked(x, above, below):
    rows = x.shape[0]
    row = lax.broadcasted_iota(jnp.int32, x.shape, 0)
    up = jnp.where(row == 0, above, pltpu.roll(x, 1, 0))
    down = jnp.where(row == rows - 1, below, pltpu.roll(x, rows - 1, 0))
    return up, down


def operator(x, up, down, weights):
    left, right = beside(x)
    diag, north, south, west, east = weights
    return diag * x - north * up - south * down - west * left - east * right


def weights_of(active, valid, grounded, active_beside, valid_beside):
    cols = active.shape[1]
    lane = lax.broadcasted_iota(jnp.int32, active.shape, 1)
    inside = (None, None, lane > 0, lane < cols - 1)
    edges = []
    for g, v, keep in zip((*active_beside, *beside(active)), (*valid_beside, *beside(valid)), inside):
        edge = 0.5 * (active + g) * valid * v
        edges.append(edge if keep is None else jnp.where(keep, edge, 0.0))
    north, south, west, east = edges
    diag = valid * (LEAKAGE + grounded) + (1.0 - valid) + north + south + west + east
    return diag, north, south, west, east


def start_kernel(
    where,
    focal_hbm,
    mask_hbm,
    current_hbm,
    cond_hbm,
    nodata_hbm,
    ground_mask_hbm,
    ground_value_hbm,
    tiles_hbm,
    field,
    pre,
    index,
    parts,
    cells,
    up_ref,
    down_ref,
    focal,
    mask,
    current,
    cond,
    nodata,
    ground_mask,
    ground_value,
    tiles,
    focal_sem,
    small_sems,
    tile_sems,
    *,
    rows,
    cols,
    pairs,
    slots,
):
    cells_of_pairs = pltpu.make_async_copy(focal_hbm, focal, focal_sem)
    cells_of_pairs.start()
    arrivals = [
        pltpu.make_async_copy(src, dst, small_sems.at[n])
        for n, (src, dst) in enumerate(
            [
                (mask_hbm, mask),
                (current_hbm, current),
                (cond_hbm, cond),
                (nodata_hbm, nodata),
                (ground_mask_hbm, ground_mask),
                (ground_value_hbm, ground_value),
            ]
        )
    ]
    for copy in arrivals:
        copy.start()
    for r in range(rows):
        pltpu.make_async_copy(tiles_hbm.at[r], tiles.at[r], tile_sems.at[r]).start()

    base_row = where[0]
    cells_of_pairs.wait()

    def listed(k, s):
        row = [lax.div(focal[end, k], cols) for end in range(2)]
        a, b = row[0] - base_row, row[1] - base_row
        near = ((a >= -2) & (a < rows + 2)) | ((b >= -2) & (b < rows + 2))
        index[k] = jnp.where(near, s, 0)

        @pl.when(near)
        def _():
            index[pairs + s] = k
            index[pairs + slots + 2 * s] = a
            index[pairs + slots + 2 * s + 1] = b
            index[pairs + 3 * slots + 2 * s] = focal[0, k] - row[0] * cols
            index[pairs + 3 * slots + 2 * s + 1] = focal[1, k] - row[1] * cols

        return s + near.astype(jnp.int32)

    count = lax.fori_loop(0, pairs, listed, jnp.int32(1))
    index[pairs + 5 * slots] = count
    chunks = (count + CHUNK - 1) // CHUNK

    for copy in arrivals:
        copy.wait()
    background = mask[...].astype(jnp.float32) * current[...]
    store(field, slice(0, rows), background)
    lane = lax.broadcasted_iota(jnp.int32, (1, TILE), 1)

    def one(s, _):
        store(field, pl.ds(s * rows, rows), background)
        for end in range(2):
            i = index[pairs + slots + 2 * s + end]
            j = index[pairs + 3 * slots + 2 * s + end]

            @pl.when((i >= 0) & (i < rows))
            def _():
                t = lax.div(j, TILE)
                at = pl.ds(s * rows + i, 1)
                sign = FOCAL_CURRENT * (1 - 2 * end)
                field[t, at, :] = field[t, at, :] + jnp.where(lane == j - t * TILE, sign, 0.0)

        return 0

    lax.fori_loop(1, count, one, 0)

    valid = (1 - nodata[...]).astype(jnp.float32)
    active = cond[...] * valid
    cells[0:rows, :] = active
    cells[rows : 2 * rows, :] = valid
    grounded = ground_mask[...].astype(jnp.float32) * ground_value[...]
    cells[2 * rows : 3 * rows, :] = grounded

    def row(r, _):
        pltpu.make_async_copy(tiles_hbm.at[r], tiles.at[r], tile_sems.at[r]).wait()
        at = pl.ds(r, CHUNK, stride=rows)
        for t in range(cols // TILE):
            pair = jnp.concatenate(cut(tiles[r, t]), axis=1)
            parts[r, t] = pair
            pre.at[t][at, :] = times_tile(field.at[t][at, :], pair)
        return 0

    lax.fori_loop(0, rows, row, 0)
    apply_tiles(field, pre, parts, rows, chunks, 1)

    for rim, first, outermost in ((up_ref, 0, 0), (down_ref, rows - 2, rows - 1)):
        two = slice(first, first + 2)
        for t in range(cols // TILE):
            lanes = slice(t * TILE, (t + 1) * TILE)
            at = 2 * pairs + t * RIM
            rim[at : at + 2, :] = pre[t, two, :]
            rim[at + 2 : at + 4, :] = active[two, lanes]
            rim[at + 4 : at + 6, :] = valid[two, lanes]
            rim[at + 6 : at + 7, :] = grounded[outermost : outermost + 1, lanes]

    def selected(s, _):
        k = index[pairs + s]
        for end in range(2):
            i = index[pairs + slots + 2 * s + end]
            j = index[pairs + 3 * slots + 2 * s + end]
            t = lax.div(j, TILE)
            for rim, first in ((up_ref, 0), (down_ref, rows - 2)):

                @pl.when((i >= first) & (i < first + 2))
                def _():
                    rim[pl.ds(end * pairs + k, 1), :] = tiles[i, t, pl.ds(j - t * TILE, 1), :]

        return 0

    lax.fori_loop(1, count, selected, 0)


def middle_kernel(
    index,
    cells,
    field,
    pre,
    parts,
    above,
    below,
    tiles_above,
    tiles_below,
    image,
    second,
    last,
    sums,
    outer,
    weights,
    rim_weights,
    one_two,
    three_four,
    *,
    rows,
    cols,
    pairs,
    slots,
):
    count = index[pairs + 5 * slots]
    chunks = (count + CHUNK - 1) // CHUNK
    active, valid, grounded = (cells[n * rows : (n + 1) * rows, :] for n in range(3))

    def told(rim, n):
        first = [2 * pairs + t * RIM + n for t in range(cols // TILE)]
        return jnp.concatenate([rim[i : i + 1, :] for i in first], axis=1)

    def own(x, i):
        return x[i : i + 1, :]

    def two(x, y):
        return jnp.concatenate([x, y], axis=0)

    active_a, active_b = (told(above, 2), told(above, 3)), (told(below, 2), told(below, 3))
    valid_a, valid_b = (told(above, 4), told(above, 5)), (told(below, 4), told(below, 5))
    all_weights = weights_of(
        active,
        valid,
        grounded,
        stacked(active, active_a[1], active_b[0]),
        stacked(valid, valid_a[1], valid_b[0]),
    )
    all_rim_weights = weights_of(
        two(active_a[1], active_b[0]),
        two(valid_a[1], valid_b[0]),
        two(told(above, 6), told(below, 6)),
        (two(active_a[0], own(active, rows - 1)), two(own(active, 0), active_b[1])),
        (two(valid_a[0], own(valid, rows - 1)), two(own(valid, 0), valid_b[1])),
    )
    for n in range(5):
        weights[n * rows : (n + 1) * rows, :] = all_weights[n]
        rim_weights[n * 8 : n * 8 + 2, :] = all_rim_weights[n]
    shared = jnp.concatenate([told(above, 0), told(above, 1), told(below, 0), told(below, 1)], axis=0)

    def first_image(s, _):
        at = s * RIM
        z = load(pre, pl.ds(s * rows, rows))
        z_two = load(outer, pl.ds(at + 1, 2))
        w = [weights[n * rows : (n + 1) * rows, :] for n in range(5)]
        store(image, pl.ds(s * rows, rows), operator(z, *stacked(z, own(z_two, 0), own(z_two, 1)), w))
        w = [rim_weights[n * 8 : n * 8 + 2, :] for n in range(5)]
        up = two(load(outer, pl.ds(at, 1)), own(z, rows - 1))
        down = two(own(z, 0), load(outer, pl.ds(at + 3, 1)))
        store(outer, pl.ds(at + 4, 2), operator(z_two, up, down, w))
        return 0

    def near(s, _):
        k = index[pairs + s]
        store(outer, pl.ds(s * RIM, 4), shared)
        for end in range(2):
            i = index[pairs + slots + 2 * s + end]
            t = lax.div(index[pairs + 3 * slots + 2 * s + end], TILE)
            sign = FOCAL_CURRENT * (1 - 2 * end)
            for rim, first, place in ((above, -2, 0), (below, rows, 2)):

                @pl.when((i >= first) & (i < first + 2))
                def _():
                    at = pl.ds(s * RIM + i - first + place, 1)
                    outer[t, at, :] = outer[t, at, :] + sign * rim[pl.ds(end * pairs + k, 1), :]

        return first_image(s, 0)

    store(outer, slice(0, 4), shared)
    first_image(0, 0)
    lax.fori_loop(1, count, near, 0)

    apply_tiles(image, second, parts, rows, chunks, 0)

    def outer_tiles(c, _):
        for tiles, row in ((tiles_above, 4), (tiles_below, 5)):
            at = pl.ds(c * (CHUNK * RIM) + row, CHUNK, stride=RIM)
            to = pl.ds(c * (CHUNK * RIM) + row + 2, CHUNK, stride=RIM)
            for t in range(cols // TILE):
                pair = jnp.concatenate(cut(tiles[0, t]), axis=1)
                outer.at[t][to, :] = times_tile(outer.at[t][at, :], pair)
        return 0

    lax.fori_loop(0, chunks, outer_tiles, 0)

    def folded(x):
        acc = x[:, 0:TILE]
        for t in range(1, cols // TILE):
            acc = acc + x[:, t * TILE : (t + 1) * TILE]
        return jnp.sum(acc, axis=0, keepdims=True)

    def four(s):
        at = pl.ds(s * rows, rows)
        w = [weights[n * rows : (n + 1) * rows, :] for n in range(5)]
        u, u_two = load(second, at), load(outer, pl.ds(s * RIM + 6, 2))
        v = operator(u, *stacked(u, own(u_two, 0), own(u_two, 1)), w)
        store(last, at, v)
        z, i = load(pre, at), load(image, at)
        return folded(load(field, at) * z), folded(z * i), folded(i * u), folded(u * v)

    a, b, c, d = four(0)
    one_two[0:pairs, :] = jnp.broadcast_to(a, (pairs, TILE))
    one_two[pairs : 2 * pairs, :] = jnp.broadcast_to(b, (pairs, TILE))
    three_four[0:pairs, :] = jnp.broadcast_to(c, (pairs, TILE))
    three_four[pairs : 2 * pairs, :] = jnp.broadcast_to(d, (pairs, TILE))

    def one(s, _):
        k = index[pairs + s]
        a, b, c, d = four(s)
        one_two[pl.ds(k, 1), :] = a
        one_two[pl.ds(pairs + k, 1), :] = b
        three_four[pl.ds(k, 1), :] = c
        three_four[pl.ds(pairs + k, 1), :] = d
        return 0

    lax.fori_loop(1, count, one, 0)
    sums[0:1, :] = jnp.sum(one_two[...].T, axis=0, keepdims=True)
    sums[1:2, :] = jnp.sum(three_four[...].T, axis=0, keepdims=True)


def finish_kernel(
    index, everyone, field, pre, image, second, last, solution, residual, first_c, second_c, *, rows, cols, pairs, block
):
    step = pl.program_id(0)

    @pl.when(step == 0)
    def _():
        total = jnp.sum(everyone[...], axis=0)
        ab, cd = total[0:1, :], total[1:2, :]
        gamma, delta = ab[:, :pairs], ab[:, pairs:]
        eta, theta = cd[:, :pairs], cd[:, pairs:]
        alpha = gamma / delta
        gamma_next = alpha * alpha * eta - gamma
        beta = 1.0 + gamma_next / gamma
        curvature = beta * beta * delta - 2.0 * beta * alpha * eta + alpha * alpha * theta
        step_next = gamma_next / curvature
        both = jnp.concatenate([alpha + step_next * beta, alpha * step_next], axis=1)
        spread = jnp.broadcast_to(both, (2 * pairs, 2 * pairs)).T
        first_c[...] = spread[:pairs, :]
        second_c[...] = spread[pairs:, :]

    def one(p, _):
        k = step * block + p
        s = index[k]
        at = pl.ds(s * rows, rows)
        a = jnp.broadcast_to(first_c[pl.ds(k, 1), :], (rows, TILE))
        b = jnp.broadcast_to(second_c[pl.ds(k, 1), :], (rows, TILE))
        for t in range(cols // TILE):
            lanes = slice(t * TILE, (t + 1) * TILE)
            solution[p, :, lanes] = a * pre[t, at, :] - b * second[t, at, :]
            residual[p, :, lanes] = field[t, at, :] - a * image[t, at, :] + b * last[t, at, :]
        return 0

    lax.fori_loop(0, block, one, 0, unroll=4)


def smem():
    return pl.BlockSpec(memory_space=pltpu.SMEM)


def vmem():
    return pl.BlockSpec(memory_space=pltpu.VMEM)


def hbm():
    return pl.BlockSpec(memory_space=pltpu.HBM)


def neighbours(up, down):
    count = lax.axis_size("space")
    ends = count - 1
    above = lax.ppermute(down, "space", [(i, (i + 1) % count) for i in range(ends)])
    below = lax.ppermute(up, "space", [((i + 1) % count, i) for i in range(ends)])
    return above, below


def on_device(conductance, nodata, ground_mask, ground_value, source_mask, source_current, tile_inverse, focal_cells):
    rows, cols = conductance.shape
    pairs = focal_cells.shape[0]
    slots = -(-(pairs + 1) // CHUNK) * CHUNK
    devices = lax.axis_size("space")
    f32 = jnp.float32
    sizes = dict(rows=rows, cols=cols, pairs=pairs, slots=slots)
    strip, fields, rim = (rows, cols), (cols // TILE, slots * rows, TILE), (2 * pairs + cols // TILE * RIM, TILE)
    per_row = tile_inverse.shape[1:]
    limit = pltpu.CompilerParams(vmem_limit_bytes=24 * MIB)
    base_row = (lax.axis_index("space") * rows).astype(jnp.int32).reshape(1)

    def shaped(shape, dtype=f32):
        return jax.ShapeDtypeStruct(shape, dtype)

    tiles_above, tiles_below = neighbours(tile_inverse[:1], tile_inverse[rows - 1 :])
    field, pre, index, parts, cells, up, down = pl.pallas_call(
        functools.partial(start_kernel, **sizes),
        in_specs=[smem(), *[hbm()] * 8],
        out_specs=[vmem(), vmem(), smem(), *[vmem()] * 4],
        out_shape=[
            shaped(fields),
            shaped(fields),
            shaped((pairs + 5 * slots + 8,), jnp.int32),
            shaped((rows, *per_row[:2], 2 * TILE), jnp.bfloat16),
            shaped((3 * rows, cols)),
            shaped(rim),
            shaped(rim),
        ],
        scratch_shapes=[
            pltpu.SMEM(focal_cells.shape[::-1], jnp.int32),
            pltpu.VMEM(strip, jnp.int32),
            pltpu.VMEM(strip, f32),
            pltpu.VMEM(strip, f32),
            pltpu.VMEM(strip, jnp.int32),
            pltpu.VMEM(strip, jnp.int32),
            pltpu.VMEM(strip, f32),
            pltpu.VMEM((rows, *per_row), f32),
            pltpu.SemaphoreType.DMA,
            pltpu.SemaphoreType.DMA((6,)),
            pltpu.SemaphoreType.DMA((rows,)),
        ],
        compiler_params=limit,
        name="start",
    )(
        base_row,
        *(
            pltpu.with_memory_space_constraint(x, pltpu.HBM)
            for x in (
                focal_cells.T,
                source_mask,
                source_current,
                conductance,
                nodata,
                ground_mask,
                ground_value,
                tile_inverse,
            )
        ),
    )
    above, below = neighbours(up, down)

    image, second, last, sums = pl.pallas_call(
        functools.partial(middle_kernel, **sizes),
        in_specs=[smem(), *[vmem()] * 8],
        out_specs=[vmem()] * 4,
        out_shape=[shaped(fields), shaped(fields), shaped(fields), shaped((2, 2 * pairs))],
        scratch_shapes=[
            pltpu.VMEM((cols // TILE, slots * RIM, TILE), f32),
            pltpu.VMEM((5 * rows, cols), f32),
            pltpu.VMEM((5 * 8, cols), f32),
            pltpu.VMEM((2 * pairs, TILE), f32),
            pltpu.VMEM((2 * pairs, TILE), f32),
        ],
        compiler_params=limit,
        name="middle",
    )(index, cells, field, pre, parts, above, below, tiles_above, tiles_below)
    copies = jnp.broadcast_to(sums, (devices, *sums.shape))
    everyone = lax.all_to_all(copies, "space", split_axis=0, concat_axis=0, tiled=True)

    block = 8
    out = jax.ShapeDtypeStruct((pairs, rows, cols), f32)
    out_block = pl.BlockSpec((block, rows, cols), lambda p: (p, 0, 0))
    return pl.pallas_call(
        functools.partial(finish_kernel, rows=rows, cols=cols, pairs=pairs, block=block),
        grid=(pairs // block,),
        in_specs=[smem(), *[vmem()] * 6],
        out_specs=[out_block, out_block],
        out_shape=[out, out],
        scratch_shapes=[pltpu.VMEM((pairs, TILE), f32), pltpu.VMEM((pairs, TILE), f32)],
        compiler_params=limit,
        name="finish",
    )(index, everyone, field, pre, image, second, last)


def solution(mesh):
    cells = P(("groups", "space"), None)
    return jax.shard_map(
        on_device,
        mesh=mesh,
        in_specs=(*[cells] * 6, P(("groups", "space"), None, None, None), P(("groups", "rhs"), None)),
        out_specs=(P("rhs", ("groups", "space"), None), P("rhs", ("groups", "space"), None)),
        check_vma=False,
    )
```

```python
import functools

import jax
import jax.numpy as jnp
from jax import lax
from jax.experimental import pallas as pl
from jax.experimental.pallas import tpu as pltpu
from jax.sharding import PartitionSpec as P

LEAKAGE = 0.05
FOCAL_CURRENT = 16.0
TILE = 128
CHUNK = 16
MIB = 1024 * 1024

RIM = 8


def cut(x):
    high = x.astype(jnp.bfloat16)
    return high, (x - high.astype(jnp.float32)).astype(jnp.bfloat16)


def load(field, at):
    return jnp.concatenate([field[t, at, :] for t in range(field.shape[0])], axis=1)


def store(field, at, x):
    for t in range(field.shape[0]):
        field[t, at, :] = x[:, t * TILE : (t + 1) * TILE]


def times_tile(x, pair):
    x_high, x_low = cut(x)
    y = jnp.dot(jnp.concatenate([x_high, x_low], axis=0), pair, preferred_element_type=jnp.float32)
    n = x.shape[0]
    return (y[:n, :TILE] + y[n:, TILE:]) + (y[n:, :TILE] + y[:n, TILE:])


def apply_tiles(src, dst, which, rows, chunks, first=0):
    def one(c, _):
        for r, parts, n in which:
            at = pl.ds(c * (CHUNK * rows) + r, CHUNK, stride=rows)
            for t in range(src.shape[0]):
                dst.at[t][at, :] = times_tile(src.at[t][at, :], parts[n, t])
        return 0

    lax.fori_loop(first, chunks, one, 0)


def keep_rows(src, dst, which, rows, chunks):
    def one(c, _):
        for r in which:
            at = pl.ds(c * (CHUNK * rows) + r, CHUNK, stride=rows)
            for t in range(src.shape[0]):
                dst.at[t][at, :] = src.at[t][at, :]
        return 0

    lax.fori_loop(0, chunks, one, 0)


def split_rows(src, dst, which, tiles_hbm, tiles, sems, parts, rows):
    for n, r in enumerate(which):
        pltpu.make_async_copy(tiles_hbm.at[r], tiles.at[n], sems.at[n]).wait()
        at = pl.ds(r, CHUNK, stride=rows)
        for t in range(src.shape[0]):
            pair = jnp.concatenate(cut(tiles[n, t]), axis=1)
            parts[n, t] = pair
            dst.at[t][at, :] = times_tile(src.at[t][at, :], pair)


def outer_rows(rows):
    return (0, 1, rows - 2, rows - 1)


def beside(x):
    cols = x.shape[1]
    return pltpu.roll(x, 1, 1), pltpu.roll(x, cols - 1, 1)


def stacked(x, above, below):
    rows = x.shape[0]
    row = lax.broadcasted_iota(jnp.int32, x.shape, 0)
    up = jnp.where(row == 0, above, pltpu.roll(x, 1, 0))
    down = jnp.where(row == rows - 1, below, pltpu.roll(x, rows - 1, 0))
    return up, down


def operator(x, up, down, weights):
    left, right = beside(x)
    diag, north, south, west, east = weights
    return diag * x - north * up - south * down - west * left - east * right


def weights_of(active, valid, grounded, active_beside, valid_beside):
    cols = active.shape[1]
    lane = lax.broadcasted_iota(jnp.int32, active.shape, 1)
    inside = (None, None, lane > 0, lane < cols - 1)
    edges = []
    for g, v, keep in zip((*active_beside, *beside(active)), (*valid_beside, *beside(valid)), inside):
        edge = 0.5 * (active + g) * valid * v
        edges.append(edge if keep is None else jnp.where(keep, edge, 0.0))
    north, south, west, east = edges
    diag = valid * (LEAKAGE + grounded) + (1.0 - valid) + north + south + west + east
    return diag, north, south, west, east


def start_kernel(
    where,
    focal_hbm,
    mask_hbm,
    current_hbm,
    cond_hbm,
    nodata_hbm,
    ground_mask_hbm,
    ground_value_hbm,
    tiles_hbm,
    field,
    pre,
    index,
    parts,
    cells,
    up_ref,
    down_ref,
    focal,
    mask,
    current,
    cond,
    nodata,
    ground_mask,
    ground_value,
    tiles,
    focal_sem,
    small_sems,
    tile_sems,
    *,
    rows,
    cols,
    pairs,
    slots,
):
    cells_of_pairs = pltpu.make_async_copy(focal_hbm, focal, focal_sem)
    cells_of_pairs.start()
    arrivals = [
        pltpu.make_async_copy(src, dst, small_sems.at[n])
        for n, (src, dst) in enumerate(
            [
                (mask_hbm, mask),
                (current_hbm, current),
                (cond_hbm, cond),
                (nodata_hbm, nodata),
                (ground_mask_hbm, ground_mask),
                (ground_value_hbm, ground_value),
            ]
        )
    ]
    for copy in arrivals:
        copy.start()
    for n, r in enumerate(outer_rows(rows)):
        pltpu.make_async_copy(tiles_hbm.at[r], tiles.at[n], tile_sems.at[n]).start()

    base_row = where[0]
    cells_of_pairs.wait()

    def listed(k, s):
        row = [lax.div(focal[end, k], cols) for end in range(2)]
        a, b = row[0] - base_row, row[1] - base_row
        near = ((a >= -2) & (a < rows + 2)) | ((b >= -2) & (b < rows + 2))
        index[k] = jnp.where(near, s, 0)

        @pl.when(near)
        def _():
            index[pairs + s] = k
            index[pairs + slots + 2 * s] = a
            index[pairs + slots + 2 * s + 1] = b
            index[pairs + 3 * slots + 2 * s] = focal[0, k] - row[0] * cols
            index[pairs + 3 * slots + 2 * s + 1] = focal[1, k] - row[1] * cols

        return s + near.astype(jnp.int32)

    count = lax.fori_loop(0, pairs, listed, jnp.int32(1))
    index[pairs + 5 * slots] = count
    chunks = (count + CHUNK - 1) // CHUNK

    for copy in arrivals:
        copy.wait()
    background = mask[...].astype(jnp.float32) * current[...]
    store(field, slice(0, rows), background)
    lane = lax.broadcasted_iota(jnp.int32, (1, TILE), 1)

    def one(s, _):
        store(field, pl.ds(s * rows, rows), background)
        for end in range(2):
            i = index[pairs + slots + 2 * s + end]
            j = index[pairs + 3 * slots + 2 * s + end]

            @pl.when((i >= 0) & (i < rows))
            def _():
                t = lax.div(j, TILE)
                at = pl.ds(s * rows + i, 1)
                sign = FOCAL_CURRENT * (1 - 2 * end)
                field[t, at, :] = field[t, at, :] + jnp.where(lane == j - t * TILE, sign, 0.0)

        return 0

    lax.fori_loop(1, count, one, 0)

    valid = (1 - nodata[...]).astype(jnp.float32)
    active = cond[...] * valid
    cells[0:rows, :] = active
    cells[rows : 2 * rows, :] = valid
    grounded = ground_mask[...].astype(jnp.float32) * ground_value[...]
    cells[2 * rows : 3 * rows, :] = grounded

    split_rows(field, pre, outer_rows(rows), tiles_hbm, tiles, tile_sems, parts, rows)
    apply_tiles(field, pre, [(r, parts, n) for n, r in enumerate(outer_rows(rows))], rows, chunks, 1)

    for rim, first, outermost in ((up_ref, 0, 0), (down_ref, rows - 2, rows - 1)):
        two = slice(first, first + 2)
        for t in range(cols // TILE):
            lanes = slice(t * TILE, (t + 1) * TILE)
            at = 2 * pairs + t * RIM
            rim[at : at + 2, :] = pre[t, two, :]
            rim[at + 2 : at + 4, :] = active[two, lanes]
            rim[at + 4 : at + 6, :] = valid[two, lanes]
            rim[at + 6 : at + 7, :] = grounded[outermost : outermost + 1, lanes]

    def selected(s, _):
        k = index[pairs + s]
        for end in range(2):
            i = index[pairs + slots + 2 * s + end]
            j = index[pairs + 3 * slots + 2 * s + end]
            t = lax.div(j, TILE)
            for rim, first, place in ((up_ref, 0, 0), (down_ref, rows - 2, 2)):

                @pl.when((i >= first) & (i < first + 2))
                def _():
                    rim[pl.ds(end * pairs + k, 1), :] = tiles[i - first + place, t, pl.ds(j - t * TILE, 1), :]

        return 0

    lax.fori_loop(1, count, selected, 0)


def inner_kernel(
    index, cells, field, parts, tiles_hbm, outer_pre, pre, second, image, tiles, inner_parts, sems, *, rows, cols, pairs, slots
):
    rest = range(2, rows - 2)
    for n, r in enumerate(rest):
        pltpu.make_async_copy(tiles_hbm.at[r], tiles.at[n], sems.at[n]).start()
    count = index[pairs + 5 * slots]
    chunks = (count + CHUNK - 1) // CHUNK
    active, valid, grounded = (cells[n * rows : (n + 1) * rows, :] for n in range(3))
    zero = jnp.zeros((1, cols), jnp.float32)
    weights = weights_of(active, valid, grounded, stacked(active, zero, zero), stacked(valid, zero, zero))

    keep_rows(outer_pre, pre, outer_rows(rows), rows, chunks)
    split_rows(field, pre, rest, tiles_hbm, tiles, sems, inner_parts, rows)
    inner = [(r, inner_parts, n) for n, r in enumerate(rest)]
    apply_tiles(field, pre, inner, rows, chunks, 1)

    def one(s, _):
        at = pl.ds(s * rows, rows)
        z = load(pre, at)
        store(image, at, operator(z, *stacked(z, zero, zero), weights))
        return 0

    lax.fori_loop(0, count, one, 0)
    apply_tiles(image, second, [(1, parts, 1), *inner, (rows - 2, parts, 2)], rows, chunks)


def middle_kernel(
    index,
    cells,
    field,
    pre,
    parts,
    above,
    below,
    tiles_above,
    tiles_below,
    inner_second,
    image,
    second,
    last,
    sums,
    outer,
    weights,
    rim_weights,
    one_two,
    three_four,
    *,
    rows,
    cols,
    pairs,
    slots,
):
    count = index[pairs + 5 * slots]
    chunks = (count + CHUNK - 1) // CHUNK
    active, valid, grounded = (cells[n * rows : (n + 1) * rows, :] for n in range(3))

    def told(rim, n):
        first = [2 * pairs + t * RIM + n for t in range(cols // TILE)]
        return jnp.concatenate([rim[i : i + 1, :] for i in first], axis=1)

    def own(x, i):
        return x[i : i + 1, :]

    def two(x, y):
        return jnp.concatenate([x, y], axis=0)

    active_a, active_b = (told(above, 2), told(above, 3)), (told(below, 2), told(below, 3))
    valid_a, valid_b = (told(above, 4), told(above, 5)), (told(below, 4), told(below, 5))
    all_weights = weights_of(
        active,
        valid,
        grounded,
        stacked(active, active_a[1], active_b[0]),
        stacked(valid, valid_a[1], valid_b[0]),
    )
    all_rim_weights = weights_of(
        two(active_a[1], active_b[0]),
        two(valid_a[1], valid_b[0]),
        two(told(above, 6), told(below, 6)),
        (two(active_a[0], own(active, rows - 1)), two(own(active, 0), active_b[1])),
        (two(valid_a[0], own(valid, rows - 1)), two(own(valid, 0), valid_b[1])),
    )
    for n in range(5):
        weights[n * rows : (n + 1) * rows, :] = all_weights[n]
        rim_weights[n * 8 : n * 8 + 2, :] = all_rim_weights[n]
    shared = jnp.concatenate([told(above, 0), told(above, 1), told(below, 0), told(below, 1)], axis=0)

    def first_image(s, _):
        at = s * RIM
        z = load(pre, pl.ds(s * rows, rows))
        z_two = load(outer, pl.ds(at + 1, 2))
        w = [weights[n * rows : (n + 1) * rows, :] for n in range(5)]
        store(image, pl.ds(s * rows, rows), operator(z, *stacked(z, own(z_two, 0), own(z_two, 1)), w))
        w = [rim_weights[n * 8 : n * 8 + 2, :] for n in range(5)]
        up = two(load(outer, pl.ds(at, 1)), own(z, rows - 1))
        down = two(own(z, 0), load(outer, pl.ds(at + 3, 1)))
        store(outer, pl.ds(at + 4, 2), operator(z_two, up, down, w))
        return 0

    def near(s, _):
        k = index[pairs + s]
        store(outer, pl.ds(s * RIM, 4), shared)
        for end in range(2):
            i = index[pairs + slots + 2 * s + end]
            t = lax.div(index[pairs + 3 * slots + 2 * s + end], TILE)
            sign = FOCAL_CURRENT * (1 - 2 * end)
            for rim, first, place in ((above, -2, 0), (below, rows, 2)):

                @pl.when((i >= first) & (i < first + 2))
                def _():
                    at = pl.ds(s * RIM + i - first + place, 1)
                    outer[t, at, :] = outer[t, at, :] + sign * rim[pl.ds(end * pairs + k, 1), :]

        return first_image(s, 0)

    store(outer, slice(0, 4), shared)
    first_image(0, 0)
    lax.fori_loop(1, count, near, 0)

    keep_rows(inner_second, second, range(1, rows - 1), rows, chunks)
    apply_tiles(image, second, [(0, parts, 0), (rows - 1, parts, 3)], rows, chunks)

    def outer_tiles(c, _):
        for tiles, row in ((tiles_above, 4), (tiles_below, 5)):
            at = pl.ds(c * (CHUNK * RIM) + row, CHUNK, stride=RIM)
            to = pl.ds(c * (CHUNK * RIM) + row + 2, CHUNK, stride=RIM)
            for t in range(cols // TILE):
                pair = jnp.concatenate(cut(tiles[0, t]), axis=1)
                outer.at[t][to, :] = times_tile(outer.at[t][at, :], pair)
        return 0

    lax.fori_loop(0, chunks, outer_tiles, 0)

    def folded(x):
        acc = x[:, 0:TILE]
        for t in range(1, cols // TILE):
            acc = acc + x[:, t * TILE : (t + 1) * TILE]
        return jnp.sum(acc, axis=0, keepdims=True)

    def four(s):
        at = pl.ds(s * rows, rows)
        w = [weights[n * rows : (n + 1) * rows, :] for n in range(5)]
        u, u_two = load(second, at), load(outer, pl.ds(s * RIM + 6, 2))
        v = operator(u, *stacked(u, own(u_two, 0), own(u_two, 1)), w)
        store(last, at, v)
        z, i = load(pre, at), load(image, at)
        return folded(load(field, at) * z), folded(z * i), folded(i * u), folded(u * v)

    a, b, c, d = four(0)
    one_two[0:pairs, :] = jnp.broadcast_to(a, (pairs, TILE))
    one_two[pairs : 2 * pairs, :] = jnp.broadcast_to(b, (pairs, TILE))
    three_four[0:pairs, :] = jnp.broadcast_to(c, (pairs, TILE))
    three_four[pairs : 2 * pairs, :] = jnp.broadcast_to(d, (pairs, TILE))

    def one(s, _):
        k = index[pairs + s]
        a, b, c, d = four(s)
        one_two[pl.ds(k, 1), :] = a
        one_two[pl.ds(pairs + k, 1), :] = b
        three_four[pl.ds(k, 1), :] = c
        three_four[pl.ds(pairs + k, 1), :] = d
        return 0

    lax.fori_loop(1, count, one, 0)
    sums[0:1, :] = jnp.sum(one_two[...].T, axis=0, keepdims=True)
    sums[1:2, :] = jnp.sum(three_four[...].T, axis=0, keepdims=True)


def finish_kernel(
    index,
    everyone,
    field,
    pre,
    image,
    second,
    last,
    solution_hbm,
    residual_hbm,
    first_c,
    second_c,
    solution,
    residual,
    solution_sems,
    residual_sems,
    *,
    rows,
    cols,
    pairs,
    block,
):
    total = jnp.sum(everyone[...], axis=0)
    ab, cd = total[0:1, :], total[1:2, :]
    gamma, delta = ab[:, :pairs], ab[:, pairs:]
    eta, theta = cd[:, :pairs], cd[:, pairs:]
    alpha = gamma / delta
    gamma_next = alpha * alpha * eta - gamma
    beta = 1.0 + gamma_next / gamma
    curvature = beta * beta * delta - 2.0 * beta * alpha * eta + alpha * alpha * theta
    step_next = gamma_next / curvature
    both = jnp.concatenate([alpha + step_next * beta, alpha * step_next], axis=1)
    spread = jnp.broadcast_to(both, (2 * pairs, 2 * pairs)).T
    first_c[...] = spread[:pairs, :]
    second_c[...] = spread[pairs:, :]

    def copies(n):
        at = pl.ds(n * block, block)
        return (
            pltpu.make_async_copy(solution.at[at], solution_hbm.at[at], solution_sems.at[n]),
            pltpu.make_async_copy(residual.at[at], residual_hbm.at[at], residual_sems.at[n]),
        )

    def one(n, _):
        for p in range(block):
            k = n * block + p
            at = pl.ds(pl.multiple_of(index[k] * rows, 8), rows)
            a = jnp.broadcast_to(first_c[pl.ds(k, 1), :], (rows, TILE))
            b = jnp.broadcast_to(second_c[pl.ds(k, 1), :], (rows, TILE))
            for t in range(cols // TILE):
                lanes = slice(t * TILE, (t + 1) * TILE)
                solution[k, :, lanes] = a * pre[t, at, :] - b * second[t, at, :]
                residual[k, :, lanes] = field[t, at, :] - a * image[t, at, :] + b * last[t, at, :]
        for copy in copies(n):
            copy.start()
        return 0

    lax.fori_loop(0, pairs // block, one, 0)

    def arrived(n, _):
        for copy in copies(n):
            copy.wait()
        return 0

    lax.fori_loop(0, pairs // block, arrived, 0)


def smem():
    return pl.BlockSpec(memory_space=pltpu.SMEM)


def vmem():
    return pl.BlockSpec(memory_space=pltpu.VMEM)


def hbm():
    return pl.BlockSpec(memory_space=pltpu.HBM)


def neighbours(up, down):
    count = lax.axis_size("space")
    ends = count - 1
    above = lax.ppermute(down, "space", [(i, (i + 1) % count) for i in range(ends)])
    below = lax.ppermute(up, "space", [((i + 1) % count, i) for i in range(ends)])
    return above, below


def on_device(conductance, nodata, ground_mask, ground_value, source_mask, source_current, tile_inverse, focal_cells):
    rows, cols = conductance.shape
    pairs = focal_cells.shape[0]
    slots = -(-(pairs + 1) // CHUNK) * CHUNK
    devices = lax.axis_size("space")
    f32 = jnp.float32
    sizes = dict(rows=rows, cols=cols, pairs=pairs, slots=slots)
    strip, fields, rim = (rows, cols), (cols // TILE, slots * rows, TILE), (2 * pairs + cols // TILE * RIM, TILE)
    per_row = tile_inverse.shape[1:]
    limit = pltpu.CompilerParams(vmem_limit_bytes=24 * MIB)
    base_row = (lax.axis_index("space") * rows).astype(jnp.int32).reshape(1)

    def shaped(shape, dtype=f32):
        return jax.ShapeDtypeStruct(shape, dtype)

    tiles_above, tiles_below = neighbours(tile_inverse[:1], tile_inverse[rows - 1 :])
    field, pre, index, parts, cells, up, down = pl.pallas_call(
        functools.partial(start_kernel, **sizes),
        in_specs=[smem(), *[hbm()] * 8],
        out_specs=[vmem(), vmem(), smem(), *[vmem()] * 4],
        out_shape=[
            shaped(fields),
            shaped(fields),
            shaped((pairs + 5 * slots + 8,), jnp.int32),
            shaped((4, *per_row[:2], 2 * TILE), jnp.bfloat16),
            shaped((3 * rows, cols)),
            shaped(rim),
            shaped(rim),
        ],
        scratch_shapes=[
            pltpu.SMEM(focal_cells.shape[::-1], jnp.int32),
            pltpu.VMEM(strip, jnp.int32),
            pltpu.VMEM(strip, f32),
            pltpu.VMEM(strip, f32),
            pltpu.VMEM(strip, jnp.int32),
            pltpu.VMEM(strip, jnp.int32),
            pltpu.VMEM(strip, f32),
            pltpu.VMEM((4, *per_row), f32),
            pltpu.SemaphoreType.DMA,
            pltpu.SemaphoreType.DMA((6,)),
            pltpu.SemaphoreType.DMA((4,)),
        ],
        compiler_params=limit,
        name="start",
    )(
        base_row,
        *(
            pltpu.with_memory_space_constraint(x, pltpu.HBM)
            for x in (
                focal_cells.T,
                source_mask,
                source_current,
                conductance,
                nodata,
                ground_mask,
                ground_value,
                tile_inverse,
            )
        ),
    )
    above, below = neighbours(up, down)

    pre, inner_second = pl.pallas_call(
        functools.partial(inner_kernel, **sizes),
        in_specs=[smem(), *[vmem()] * 3, hbm(), vmem()],
        out_specs=[vmem()] * 2,
        out_shape=[shaped(fields)] * 2,
        scratch_shapes=[
            pltpu.VMEM(fields, f32),
            pltpu.VMEM((rows - 4, *per_row), f32),
            pltpu.VMEM((rows - 4, *per_row[:2], 2 * TILE), jnp.bfloat16),
            pltpu.SemaphoreType.DMA((rows - 4,)),
        ],
        compiler_params=limit,
        name="inner",
    )(index, cells, field, parts, pltpu.with_memory_space_constraint(tile_inverse, pltpu.HBM), pre)

    image, second, last, sums = pl.pallas_call(
        functools.partial(middle_kernel, **sizes),
        in_specs=[smem(), *[vmem()] * 9],
        out_specs=[vmem()] * 4,
        out_shape=[*[shaped(fields)] * 3, shaped((2, 2 * pairs))],
        scratch_shapes=[
            pltpu.VMEM((cols // TILE, slots * RIM, TILE), f32),
            pltpu.VMEM((5 * rows, cols), f32),
            pltpu.VMEM((5 * 8, cols), f32),
            pltpu.VMEM((2 * pairs, TILE), f32),
            pltpu.VMEM((2 * pairs, TILE), f32),
        ],
        compiler_params=limit,
        name="middle",
    )(index, cells, field, pre, parts, above, below, tiles_above, tiles_below, inner_second)
    copies = jnp.broadcast_to(sums, (devices, *sums.shape))
    everyone = lax.all_to_all(copies, "space", split_axis=0, concat_axis=0, tiled=True)

    block = 8
    out = (pairs, rows, cols)
    return pl.pallas_call(
        functools.partial(finish_kernel, rows=rows, cols=cols, pairs=pairs, block=block),
        in_specs=[smem(), *[vmem()] * 6],
        out_specs=[hbm()] * 2,
        out_shape=[shaped(out)] * 2,
        scratch_shapes=[
            pltpu.VMEM((pairs, TILE), f32),
            pltpu.VMEM((pairs, TILE), f32),
            pltpu.VMEM(out, f32),
            pltpu.VMEM(out, f32),
            pltpu.SemaphoreType.DMA((pairs // block,)),
            pltpu.SemaphoreType.DMA((pairs // block,)),
        ],
        compiler_params=limit,
        name="finish",
    )(index, everyone, field, pre, image, second, last)


def solution(mesh):
    cells = P(("groups", "space"), None)
    return jax.shard_map(
        on_device,
        mesh=mesh,
        in_specs=(*[cells] * 6, P(("groups", "space"), None, None, None), P(("groups", "rhs"), None)),
        out_specs=(P("rhs", ("groups", "space"), None), P("rhs", ("groups", "space"), None)),
        check_vma=False,
    )
```

```python
import functools

import jax
import jax.numpy as jnp
from jax import lax
from jax.experimental import pallas as pl
from jax.experimental.pallas import tpu as pltpu
from jax.sharding import PartitionSpec as P

LEAKAGE = 0.05
FOCAL_CURRENT = 16.0
TILE = 128
CHUNK = 16
GROUP = 4
MIB = 1024 * 1024

RIM = 8


def cut(x):
    high = x.astype(jnp.bfloat16)
    return high, (x - high.astype(jnp.float32)).astype(jnp.bfloat16)


def load(field, at):
    return jnp.concatenate([field[t, at, :] for t in range(field.shape[0])], axis=1)


def store(field, at, x):
    for t in range(field.shape[0]):
        field[t, at, :] = x[:, t * TILE : (t + 1) * TILE]


def times_tile(x, pair):
    x_high, x_low = cut(x)
    y = jnp.dot(jnp.concatenate([x_high, x_low], axis=0), pair, preferred_element_type=jnp.float32)
    n = x.shape[0]
    return (y[:n, :TILE] + y[n:, TILE:]) + (y[n:, :TILE] + y[:n, TILE:])


def apply_tiles(src, dst, which, rows, chunks, first=0):
    def one(c, _):
        for r, parts, n in which:
            at = pl.ds(c * (CHUNK * rows) + r, CHUNK, stride=rows)
            for t in range(src.shape[0]):
                dst.at[t][at, :] = times_tile(src.at[t][at, :], parts[n, t])
        return 0

    lax.fori_loop(first, chunks, one, 0)


def keep_rows(src, dst, which, rows, chunks, first=0):
    def one(c, _):
        for r in which:
            at = pl.ds(c * (CHUNK * rows) + r, CHUNK, stride=rows)
            for t in range(src.shape[0]):
                dst.at[t][at, :] = src.at[t][at, :]
        return 0

    lax.fori_loop(first, chunks, one, 0)


def split_rows(src, dst, which, tiles_hbm, tiles, sems, parts, rows):
    for n, r in enumerate(which):
        pltpu.make_async_copy(tiles_hbm.at[r], tiles.at[n], sems.at[n]).wait()
        at = pl.ds(r, CHUNK, stride=rows)
        for t in range(src.shape[0]):
            pair = jnp.concatenate(cut(tiles[n, t]), axis=1)
            parts[n, t] = pair
            dst.at[t][at, :] = times_tile(src.at[t][at, :], pair)


def outer_rows(rows):
    return (0, 1, rows - 2, rows - 1)


def beside(x):
    cols = x.shape[1]
    return pltpu.roll(x, 1, 1), pltpu.roll(x, cols - 1, 1)


def stacked(x, above, below):
    rows = x.shape[0]
    row = lax.broadcasted_iota(jnp.int32, x.shape, 0)
    up = jnp.where(row == 0, above, pltpu.roll(x, 1, 0))
    down = jnp.where(row == rows - 1, below, pltpu.roll(x, rows - 1, 0))
    return up, down


def operator(x, up, down, weights):
    left, right = beside(x)
    diag, north, south, west, east = weights
    return diag * x - north * up - south * down - west * left - east * right


def weights_of(active, valid, grounded, active_beside, valid_beside):
    cols = active.shape[1]
    lane = lax.broadcasted_iota(jnp.int32, active.shape, 1)
    inside = (None, None, lane > 0, lane < cols - 1)
    edges = []
    for g, v, keep in zip((*active_beside, *beside(active)), (*valid_beside, *beside(valid)), inside):
        edge = 0.5 * (active + g) * valid * v
        edges.append(edge if keep is None else jnp.where(keep, edge, 0.0))
    north, south, west, east = edges
    diag = valid * (LEAKAGE + grounded) + (1.0 - valid) + north + south + west + east
    return diag, north, south, west, east


def start_kernel(
    where,
    focal_hbm,
    mask_hbm,
    current_hbm,
    cond_hbm,
    nodata_hbm,
    ground_mask_hbm,
    ground_value_hbm,
    tiles_hbm,
    field,
    pre,
    index,
    parts,
    cells,
    up_ref,
    down_ref,
    focal,
    mask,
    current,
    cond,
    nodata,
    ground_mask,
    ground_value,
    tiles,
    focal_sem,
    small_sems,
    tile_sems,
    *,
    rows,
    cols,
    pairs,
    slots,
):
    cells_of_pairs = pltpu.make_async_copy(focal_hbm, focal, focal_sem)
    cells_of_pairs.start()
    arrivals = [
        pltpu.make_async_copy(src, dst, small_sems.at[n])
        for n, (src, dst) in enumerate(
            [
                (mask_hbm, mask),
                (current_hbm, current),
                (cond_hbm, cond),
                (nodata_hbm, nodata),
                (ground_mask_hbm, ground_mask),
                (ground_value_hbm, ground_value),
            ]
        )
    ]
    for copy in arrivals:
        copy.start()
    for n, r in enumerate(outer_rows(rows)):
        pltpu.make_async_copy(tiles_hbm.at[r], tiles.at[n], tile_sems.at[n]).start()

    base_row = where[0]
    cells_of_pairs.wait()

    def is_near(cell):
        return (cell >= (base_row - 2) * cols) & (cell < (base_row + rows + 2) * cols)

    def listed(k, s):
        near = is_near(focal[0, k]) | is_near(focal[1, k])
        index[k] = jnp.where(near, s, 0)
        index[pairs + s] = k
        return s + near.astype(jnp.int32)

    index[pairs] = pairs
    count = lax.fori_loop(0, pairs, listed, jnp.int32(1), unroll=8)
    index[pairs + 5 * slots] = count
    for n in range(GROUP):
        index[pairs + count + n] = pairs
    chunks = (count + CHUNK - 1) // CHUNK

    for copy in arrivals:
        copy.wait()
    background = mask[...].astype(jnp.float32) * current[...]
    store(field, slice(0, rows), background)
    lane = lax.broadcasted_iota(jnp.int32, (1, TILE), 1)

    def one(s, _):
        store(field, pl.ds(s * rows, rows), background)
        for end in range(2):
            cell = focal[end, index[pairs + s]]
            i = lax.div(cell, cols)
            j = cell - i * cols
            i = i - base_row
            index[pairs + slots + 2 * s + end] = i
            index[pairs + 3 * slots + 2 * s + end] = j

            @pl.when((i >= 0) & (i < rows))
            def _():
                t = lax.div(j, TILE)
                at = pl.ds(s * rows + i, 1)
                sign = FOCAL_CURRENT * (1 - 2 * end)
                field[t, at, :] = field[t, at, :] + jnp.where(lane == j - t * TILE, sign, 0.0)

        return 0

    lax.fori_loop(1, count, one, 0)

    valid = (1 - nodata[...]).astype(jnp.float32)
    active = cond[...] * valid
    cells[0:rows, :] = active
    cells[rows : 2 * rows, :] = valid
    grounded = ground_mask[...].astype(jnp.float32) * ground_value[...]
    cells[2 * rows : 3 * rows, :] = grounded

    split_rows(field, pre, outer_rows(rows), tiles_hbm, tiles, tile_sems, parts, rows)
    apply_tiles(field, pre, [(r, parts, n) for n, r in enumerate(outer_rows(rows))], rows, chunks, 1)

    for rim, first, outermost in ((up_ref, 0, 0), (down_ref, rows - 2, rows - 1)):
        two = slice(first, first + 2)
        for t in range(cols // TILE):
            lanes = slice(t * TILE, (t + 1) * TILE)
            at = 2 * pairs + t * RIM
            rim[at : at + 2, :] = pre[t, two, :]
            rim[at + 2 : at + 4, :] = active[two, lanes]
            rim[at + 4 : at + 6, :] = valid[two, lanes]
            rim[at + 6 : at + 7, :] = grounded[outermost : outermost + 1, lanes]

    def selected(s, _):
        k = index[pairs + s]
        for end in range(2):
            i = index[pairs + slots + 2 * s + end]
            j = index[pairs + 3 * slots + 2 * s + end]
            t = lax.div(j, TILE)
            for rim, first, place in ((up_ref, 0, 0), (down_ref, rows - 2, 2)):

                @pl.when((i >= first) & (i < first + 2))
                def _():
                    rim[pl.ds(end * pairs + k, 1), :] = tiles[i - first + place, t, pl.ds(j - t * TILE, 1), :]

        return 0

    lax.fori_loop(1, count, selected, 0)


def inner_kernel(
    index, cells, field, parts, tiles_hbm, outer_pre, pre, second, image, tiles, inner_parts, sems, *, rows, cols, pairs, slots
):
    rest = range(2, rows - 2)
    for n, r in enumerate(rest):
        pltpu.make_async_copy(tiles_hbm.at[r], tiles.at[n], sems.at[n]).start()
    count = index[pairs + 5 * slots]
    chunks = (count + CHUNK - 1) // CHUNK
    active, valid, grounded = (cells[n * rows : (n + 1) * rows, :] for n in range(3))
    zero = jnp.zeros((1, cols), jnp.float32)
    weights = weights_of(active, valid, grounded, stacked(active, zero, zero), stacked(valid, zero, zero))

    keep_rows(outer_pre, pre, outer_rows(rows), rows, chunks)
    split_rows(field, pre, rest, tiles_hbm, tiles, sems, inner_parts, rows)
    inner = [(r, inner_parts, n) for n, r in enumerate(rest)]
    apply_tiles(field, pre, inner, rows, chunks, 1)

    def one(s, _):
        at = pl.ds(s * rows, rows)
        z = load(pre, at)
        store(image, at, operator(z, *stacked(z, zero, zero), weights))
        return 0

    lax.fori_loop(0, count, one, 0)
    apply_tiles(image, second, [(1, parts, 1), *inner, (rows - 2, parts, 2)], rows, chunks)


def middle_kernel(
    index,
    cells,
    field,
    pre,
    parts,
    above,
    below,
    tiles_above,
    tiles_below,
    inner_second,
    image,
    second,
    last,
    sums,
    outer,
    weights,
    rim_weights,
    kept_sem,
    *by_pair,
    rows,
    cols,
    pairs,
    slots,
):
    first_chunk = pl.ds(0, CHUNK * rows)
    kept = pltpu.make_async_copy(inner_second.at[:, first_chunk, :], second.at[:, first_chunk, :], kept_sem)
    kept.start()
    count = index[pairs + 5 * slots]
    chunks = (count + CHUNK - 1) // CHUNK
    active, valid, grounded = (cells[n * rows : (n + 1) * rows, :] for n in range(3))

    def told(rim, n):
        first = [2 * pairs + t * RIM + n for t in range(cols // TILE)]
        return jnp.concatenate([rim[i : i + 1, :] for i in first], axis=1)

    def own(x, i):
        return x[i : i + 1, :]

    def two(x, y):
        return jnp.concatenate([x, y], axis=0)

    active_a, active_b = (told(above, 2), told(above, 3)), (told(below, 2), told(below, 3))
    valid_a, valid_b = (told(above, 4), told(above, 5)), (told(below, 4), told(below, 5))
    all_weights = weights_of(
        active,
        valid,
        grounded,
        stacked(active, active_a[1], active_b[0]),
        stacked(valid, valid_a[1], valid_b[0]),
    )
    all_rim_weights = weights_of(
        two(active_a[1], active_b[0]),
        two(valid_a[1], valid_b[0]),
        two(told(above, 6), told(below, 6)),
        (two(active_a[0], own(active, rows - 1)), two(own(active, 0), active_b[1])),
        (two(valid_a[0], own(valid, rows - 1)), two(own(valid, 0), valid_b[1])),
    )
    for n in range(5):
        weights[n * rows : (n + 1) * rows, :] = all_weights[n]
        rim_weights[n * 8 : n * 8 + 2, :] = all_rim_weights[n]
    shared = jnp.concatenate([told(above, 0), told(above, 1), told(below, 0), told(below, 1)], axis=0)

    def near(s, _):
        k = index[pairs + s]
        store(outer, pl.ds(s * RIM, 4), shared)
        for end in range(2):
            i = index[pairs + slots + 2 * s + end]
            t = lax.div(index[pairs + 3 * slots + 2 * s + end], TILE)
            sign = FOCAL_CURRENT * (1 - 2 * end)
            for rim, first, place in ((above, -2, 0), (below, rows, 2)):

                @pl.when((i >= first) & (i < first + 2))
                def _():
                    at = pl.ds(s * RIM + i - first + place, 1)
                    outer[t, at, :] = outer[t, at, :] + sign * rim[pl.ds(end * pairs + k, 1), :]

        return 0

    store(outer, slice(0, 4), shared)
    lax.fori_loop(1, count, near, 0)

    def first_image(g, _):
        for s in [g * GROUP + n for n in range(GROUP)]:
            at = s * RIM
            z = load(pre, pl.ds(s * rows, rows))
            z_two = load(outer, pl.ds(at + 1, 2))
            w = [weights[n * rows : (n + 1) * rows, :] for n in range(5)]
            store(image, pl.ds(s * rows, rows), operator(z, *stacked(z, own(z_two, 0), own(z_two, 1)), w))
            w = [rim_weights[n * 8 : n * 8 + 2, :] for n in range(5)]
            up = two(load(outer, pl.ds(at, 1)), own(z, rows - 1))
            down = two(own(z, 0), load(outer, pl.ds(at + 3, 1)))
            store(outer, pl.ds(at + 4, 2), operator(z_two, up, down, w))
        return 0

    groups = (count + GROUP - 1) // GROUP
    lax.fori_loop(0, groups, first_image, 0)

    kept.wait()
    keep_rows(inner_second, second, range(1, rows - 1), rows, chunks, 1)

    def outer_tiles(c, _):
        for tiles, row in ((tiles_above, 4), (tiles_below, 5)):
            at = pl.ds(c * (CHUNK * RIM) + row, CHUNK, stride=RIM)
            to = pl.ds(c * (CHUNK * RIM) + row + 2, CHUNK, stride=RIM)
            for t in range(cols // TILE):
                pair = jnp.concatenate(cut(tiles[0, t]), axis=1)
                outer.at[t][to, :] = times_tile(outer.at[t][at, :], pair)
        for r, n in ((0, 0), (rows - 1, 3)):
            at = pl.ds(c * (CHUNK * rows) + r, CHUNK, stride=rows)
            for t in range(cols // TILE):
                second.at[t][at, :] = times_tile(image.at[t][at, :], parts[n, t])
        return 0

    lax.fori_loop(0, chunks, outer_tiles, 0)

    def folded(x):
        acc = x[:, 0:TILE]
        for t in range(1, cols // TILE):
            acc = acc + x[:, t * TILE : (t + 1) * TILE]
        return jnp.sum(acc, axis=0, keepdims=True)

    def four(s):
        at = pl.ds(s * rows, rows)
        w = [weights[n * rows : (n + 1) * rows, :] for n in range(5)]
        u, u_two = load(second, at), load(outer, pl.ds(s * RIM + 6, 2))
        v = operator(u, *stacked(u, own(u_two, 0), own(u_two, 1)), w)
        store(last, at, v)
        z, i = load(pre, at), load(image, at)
        return folded(load(field, at) * z), folded(z * i), folded(i * u), folded(u * v)

    def group(g, shared):
        members = [g * GROUP + n for n in range(GROUP)]
        sums_of = [four(s) for s in members]
        if shared:
            for part, x in zip(by_pair, sums_of[0]):
                part[...] = jnp.broadcast_to(x, part.shape)
        for s, four_sums in zip(members, sums_of):
            for part, x in zip(by_pair, four_sums):
                part[pl.ds(index[pairs + s], 1), :] = x

    def later(g, _):
        group(g, False)
        return 0

    group(0, True)
    lax.fori_loop(1, groups, later, 0)
    for n in range(2):
        both = jnp.concatenate([by_pair[2 * n + m][0:pairs, :] for m in range(2)], axis=0)
        sums[n : n + 1, :] = jnp.sum(both.T, axis=0, keepdims=True)


def finish_kernel(
    index,
    everyone,
    field,
    pre,
    image,
    second,
    last,
    solution_hbm,
    residual_hbm,
    first_c,
    second_c,
    solution,
    residual,
    solution_sems,
    residual_sems,
    *,
    rows,
    cols,
    pairs,
    block,
):
    total = jnp.sum(everyone[...], axis=0)
    ab, cd = total[0:1, :], total[1:2, :]
    gamma, delta = ab[:, :pairs], ab[:, pairs:]
    eta, theta = cd[:, :pairs], cd[:, pairs:]
    alpha = gamma / delta
    gamma_next = alpha * alpha * eta - gamma
    beta = 1.0 + gamma_next / gamma
    curvature = beta * beta * delta - 2.0 * beta * alpha * eta + alpha * alpha * theta
    step_next = gamma_next / curvature
    both = jnp.concatenate([alpha + step_next * beta, alpha * step_next], axis=1)
    spread = jnp.broadcast_to(both, (2 * pairs, 2 * pairs)).T
    first_c[...] = spread[:pairs, :]
    second_c[...] = spread[pairs:, :]

    def copies(n):
        at = pl.ds(n * block, block)
        return (
            pltpu.make_async_copy(solution.at[at], solution_hbm.at[at], solution_sems.at[n]),
            pltpu.make_async_copy(residual.at[at], residual_hbm.at[at], residual_sems.at[n]),
        )

    def one(n, _):
        for p in range(block):
            k = n * block + p
            at = pl.ds(pl.multiple_of(index[k] * rows, 8), rows)
            a = jnp.broadcast_to(first_c[pl.ds(k, 1), :], (rows, TILE))
            b = jnp.broadcast_to(second_c[pl.ds(k, 1), :], (rows, TILE))
            for t in range(cols // TILE):
                lanes = slice(t * TILE, (t + 1) * TILE)
                solution[k, :, lanes] = a * pre[t, at, :] - b * second[t, at, :]
                residual[k, :, lanes] = field[t, at, :] - a * image[t, at, :] + b * last[t, at, :]
        for copy in copies(n):
            copy.start()
        return 0

    lax.fori_loop(0, pairs // block, one, 0)

    def arrived(n, _):
        for copy in copies(n):
            copy.wait()
        return 0

    lax.fori_loop(0, pairs // block, arrived, 0)


def smem():
    return pl.BlockSpec(memory_space=pltpu.SMEM)


def vmem():
    return pl.BlockSpec(memory_space=pltpu.VMEM)


def hbm():
    return pl.BlockSpec(memory_space=pltpu.HBM)


def neighbours(up, down):
    count = lax.axis_size("space")
    ends = count - 1
    above = lax.ppermute(down, "space", [(i, (i + 1) % count) for i in range(ends)])
    below = lax.ppermute(up, "space", [((i + 1) % count, i) for i in range(ends)])
    return above, below


def on_device(conductance, nodata, ground_mask, ground_value, source_mask, source_current, tile_inverse, focal_cells):
    rows, cols = conductance.shape
    pairs = focal_cells.shape[0]
    slots = -(-(pairs + 1) // CHUNK) * CHUNK
    devices = lax.axis_size("space")
    f32 = jnp.float32
    sizes = dict(rows=rows, cols=cols, pairs=pairs, slots=slots)
    strip, fields, rim = (rows, cols), (cols // TILE, slots * rows, TILE), (2 * pairs + cols // TILE * RIM, TILE)
    per_row = tile_inverse.shape[1:]
    limit = pltpu.CompilerParams(vmem_limit_bytes=24 * MIB)
    base_row = (lax.axis_index("space") * rows).astype(jnp.int32).reshape(1)

    def shaped(shape, dtype=f32):
        return jax.ShapeDtypeStruct(shape, dtype)

    tiles_above, tiles_below = neighbours(tile_inverse[:1], tile_inverse[rows - 1 :])
    field, pre, index, parts, cells, up, down = pl.pallas_call(
        functools.partial(start_kernel, **sizes),
        in_specs=[smem(), *[hbm()] * 8],
        out_specs=[vmem(), vmem(), smem(), *[vmem()] * 4],
        out_shape=[
            shaped(fields),
            shaped(fields),
            shaped((pairs + 5 * slots + 8,), jnp.int32),
            shaped((4, *per_row[:2], 2 * TILE), jnp.bfloat16),
            shaped((3 * rows, cols)),
            shaped(rim),
            shaped(rim),
        ],
        scratch_shapes=[
            pltpu.SMEM(focal_cells.shape[::-1], jnp.int32),
            pltpu.VMEM(strip, jnp.int32),
            pltpu.VMEM(strip, f32),
            pltpu.VMEM(strip, f32),
            pltpu.VMEM(strip, jnp.int32),
            pltpu.VMEM(strip, jnp.int32),
            pltpu.VMEM(strip, f32),
            pltpu.VMEM((4, *per_row), f32),
            pltpu.SemaphoreType.DMA,
            pltpu.SemaphoreType.DMA((6,)),
            pltpu.SemaphoreType.DMA((4,)),
        ],
        compiler_params=limit,
        name="start",
    )(
        base_row,
        *(
            pltpu.with_memory_space_constraint(x, pltpu.HBM)
            for x in (
                focal_cells.T,
                source_mask,
                source_current,
                conductance,
                nodata,
                ground_mask,
                ground_value,
                tile_inverse,
            )
        ),
    )
    above, below = neighbours(up, down)

    pre, inner_second = pl.pallas_call(
        functools.partial(inner_kernel, **sizes),
        in_specs=[smem(), *[vmem()] * 3, hbm(), vmem()],
        out_specs=[vmem()] * 2,
        out_shape=[shaped(fields)] * 2,
        scratch_shapes=[
            pltpu.VMEM(fields, f32),
            pltpu.VMEM((rows - 4, *per_row), f32),
            pltpu.VMEM((rows - 4, *per_row[:2], 2 * TILE), jnp.bfloat16),
            pltpu.SemaphoreType.DMA((rows - 4,)),
        ],
        compiler_params=limit,
        name="inner",
    )(index, cells, field, parts, pltpu.with_memory_space_constraint(tile_inverse, pltpu.HBM), pre)

    image, second, last, sums = pl.pallas_call(
        functools.partial(middle_kernel, **sizes),
        in_specs=[smem(), *[vmem()] * 9],
        out_specs=[vmem()] * 4,
        out_shape=[*[shaped(fields)] * 3, shaped((2, 2 * pairs))],
        scratch_shapes=[
            pltpu.VMEM((cols // TILE, slots * RIM, TILE), f32),
            pltpu.VMEM((5 * rows, cols), f32),
            pltpu.VMEM((5 * 8, cols), f32),
            pltpu.SemaphoreType.DMA,
            *[pltpu.VMEM((pairs + 8, TILE), f32)] * 4,
        ],
        compiler_params=limit,
        name="middle",
    )(index, cells, field, pre, parts, above, below, tiles_above, tiles_below, inner_second)
    copies = jnp.broadcast_to(sums, (devices, *sums.shape))
    everyone = lax.all_to_all(copies, "space", split_axis=0, concat_axis=0, tiled=True)

    block = 8
    out = (pairs, rows, cols)
    return pl.pallas_call(
        functools.partial(finish_kernel, rows=rows, cols=cols, pairs=pairs, block=block),
        in_specs=[smem(), *[vmem()] * 6],
        out_specs=[hbm()] * 2,
        out_shape=[shaped(out)] * 2,
        scratch_shapes=[
            pltpu.VMEM((pairs, TILE), f32),
            pltpu.VMEM((pairs, TILE), f32),
            pltpu.VMEM(out, f32),
            pltpu.VMEM(out, f32),
            pltpu.SemaphoreType.DMA((pairs // block,)),
            pltpu.SemaphoreType.DMA((pairs // block,)),
        ],
        compiler_params=limit,
        name="finish",
    )(index, everyone, field, pre, image, second, last)


def solution(mesh):
    cells = P(("groups", "space"), None)
    return jax.shard_map(
        on_device,
        mesh=mesh,
        in_specs=(*[cells] * 6, P(("groups", "space"), None, None, None), P(("groups", "rhs"), None)),
        out_specs=(P("rhs", ("groups", "space"), None), P("rhs", ("groups", "space"), None)),
        check_vma=False,
    )
```

```python
import functools

import jax
import jax.numpy as jnp
from jax import lax
from jax.experimental import pallas as pl
from jax.experimental.pallas import tpu as pltpu
from jax.sharding import PartitionSpec as P

LEAKAGE = 0.05
FOCAL_CURRENT = 16.0
TILE = 128
HALF = TILE // 2
CHUNK = 16
GROUP = 4
MIB = 1024 * 1024

RIM = 8


def cut(x):
    high = x.astype(jnp.bfloat16)
    return high, (x - high.astype(jnp.float32)).astype(jnp.bfloat16)


def load(field, at):
    return jnp.concatenate([field[t, at, :] for t in range(field.shape[0])], axis=1)


def store(field, at, x):
    for t in range(field.shape[0]):
        field[t, at, :] = x[:, t * TILE : (t + 1) * TILE]


def times_tile(x, pair):
    x_high, x_low = cut(x)
    y = jnp.dot(jnp.concatenate([x_high, x_low], axis=0), pair, preferred_element_type=jnp.float32)
    n = x.shape[0]
    return (y[:n, :TILE] + y[n:, TILE:]) + (y[n:, :TILE] + y[:n, TILE:])


def apply_tiles(src, dst, which, rows, chunks, first=0):
    def one(c, _):
        for r, parts, n in which:
            at = pl.ds(c * (CHUNK * rows) + r, CHUNK, stride=rows)
            for t in range(src.shape[0]):
                dst.at[t][at, :] = times_tile(src.at[t][at, :], parts[n, t])
        return 0

    lax.fori_loop(first, chunks, one, 0)


def keep_rows(src, dst, which, rows, chunks, first=0):
    def one(c, _):
        for r in which:
            at = pl.ds(c * (CHUNK * rows) + r, CHUNK, stride=rows)
            for t in range(src.shape[0]):
                dst.at[t][at, :] = src.at[t][at, :]
        return 0

    lax.fori_loop(first, chunks, one, 0)


def split_rows(src, dst, which, tiles_hbm, tiles, sems, parts, rows):
    for n, r in enumerate(which):
        pltpu.make_async_copy(tiles_hbm.at[r], tiles.at[n], sems.at[n]).wait()
        at = pl.ds(r, CHUNK, stride=rows)
        for t in range(src.shape[0]):
            pair = jnp.concatenate(cut(tiles[n, t]), axis=1)
            parts[n, t] = pair
            dst.at[t][at, :] = times_tile(src.at[t][at, :], pair)


def outer_rows(rows):
    return (0, 1, rows - 2, rows - 1)


def beside(x):
    cols = x.shape[1]
    return pltpu.roll(x, 1, 1), pltpu.roll(x, cols - 1, 1)


def stacked(x, above, below):
    rows = x.shape[0]
    row = lax.broadcasted_iota(jnp.int32, x.shape, 0)
    up = jnp.where(row == 0, above, pltpu.roll(x, 1, 0))
    down = jnp.where(row == rows - 1, below, pltpu.roll(x, rows - 1, 0))
    return up, down


def operator(x, up, down, weights):
    left, right = beside(x)
    diag, north, south, west, east = weights
    return diag * x - north * up - south * down - west * left - east * right


def weights_of(active, valid, grounded, active_beside, valid_beside):
    cols = active.shape[1]
    lane = lax.broadcasted_iota(jnp.int32, active.shape, 1)
    inside = (None, None, lane > 0, lane < cols - 1)
    edges = []
    for g, v, keep in zip((*active_beside, *beside(active)), (*valid_beside, *beside(valid)), inside):
        edge = 0.5 * (active + g) * valid * v
        edges.append(edge if keep is None else jnp.where(keep, edge, 0.0))
    north, south, west, east = edges
    diag = valid * (LEAKAGE + grounded) + (1.0 - valid) + north + south + west + east
    return diag, north, south, west, east


def below_diagonal():
    row = lax.broadcasted_iota(jnp.int32, (HALF, TILE), 0)
    lane = lax.broadcasted_iota(jnp.int32, (HALF, TILE), 1)
    return lane < row, lane == row + HALF


def pack_kernel(tiles_hbm, up_ref, down_ref, tiles, sems, *, rows):
    copies = [pltpu.make_async_copy(tiles_hbm.at[r], tiles.at[n], sems.at[n]) for n, r in enumerate((0, rows - 1))]
    for copy in copies:
        copy.start()
    moved, diagonal = below_diagonal()
    count = tiles.shape[1]
    for n, packed in enumerate((up_ref, down_ref)):
        copies[n].wait()
        for t in range(count):
            upper, lower = tiles[n, t, :HALF, :], tiles[n, t, HALF:, :]
            packed[t * HALF : (t + 1) * HALF, :] = jnp.where(moved, pltpu.roll(lower, HALF, 1), upper)
            at = count * HALF + t
            packed[at : at + 1, :] = jnp.sum(jnp.where(diagonal, lower, 0.0), axis=0, keepdims=True)


def unpacked(packed, t, count):
    x = packed[t * HALF : (t + 1) * HALF, :]
    diagonal = packed[count * HALF + t : count * HALF + t + 1, :]
    moved, _ = below_diagonal()
    top = jnp.where(moved, 0.0, x)
    bottom = pltpu.roll(jnp.where(moved, x, 0.0), HALF, 1)
    half = jnp.concatenate([top, bottom], axis=0)
    row = lax.broadcasted_iota(jnp.int32, (TILE, TILE), 0)
    lane = lax.broadcasted_iota(jnp.int32, (TILE, TILE), 1)
    return jnp.where(row == lane, jnp.where(row < HALF, half, diagonal), half + half.T)


def start_kernel(
    where,
    focal_hbm,
    mask_hbm,
    current_hbm,
    cond_hbm,
    nodata_hbm,
    ground_mask_hbm,
    ground_value_hbm,
    tiles_hbm,
    field,
    pre,
    index,
    parts,
    cells,
    up_ref,
    down_ref,
    focal,
    mask,
    current,
    cond,
    nodata,
    ground_mask,
    ground_value,
    tiles,
    focal_sem,
    small_sems,
    tile_sems,
    *,
    rows,
    cols,
    pairs,
    slots,
):
    cells_of_pairs = pltpu.make_async_copy(focal_hbm, focal, focal_sem)
    cells_of_pairs.start()
    arrivals = [
        pltpu.make_async_copy(src, dst, small_sems.at[n])
        for n, (src, dst) in enumerate(
            [
                (mask_hbm, mask),
                (current_hbm, current),
                (cond_hbm, cond),
                (nodata_hbm, nodata),
                (ground_mask_hbm, ground_mask),
                (ground_value_hbm, ground_value),
            ]
        )
    ]
    for copy in arrivals:
        copy.start()
    for n, r in enumerate(outer_rows(rows)):
        pltpu.make_async_copy(tiles_hbm.at[r], tiles.at[n], tile_sems.at[n]).start()

    base_row = where[0]
    cells_of_pairs.wait()

    def is_near(cell):
        return (cell >= (base_row - 2) * cols) & (cell < (base_row + rows + 2) * cols)

    def listed(k, s):
        near = is_near(focal[0, k]) | is_near(focal[1, k])
        index[k] = jnp.where(near, s, 0)
        index[pairs + s] = k
        return s + near.astype(jnp.int32)

    index[pairs] = pairs
    count = lax.fori_loop(0, pairs, listed, jnp.int32(1), unroll=8)
    index[pairs + 5 * slots] = count
    for n in range(GROUP):
        index[pairs + count + n] = pairs
    chunks = (count + CHUNK - 1) // CHUNK

    for copy in arrivals:
        copy.wait()
    background = mask[...].astype(jnp.float32) * current[...]
    store(field, slice(0, rows), background)
    lane = lax.broadcasted_iota(jnp.int32, (1, TILE), 1)

    def one(s, _):
        store(field, pl.ds(s * rows, rows), background)
        for end in range(2):
            cell = focal[end, index[pairs + s]]
            i = lax.div(cell, cols)
            j = cell - i * cols
            i = i - base_row
            index[pairs + slots + 2 * s + end] = i
            index[pairs + 3 * slots + 2 * s + end] = j

            @pl.when((i >= 0) & (i < rows))
            def _():
                t = lax.div(j, TILE)
                at = pl.ds(s * rows + i, 1)
                sign = FOCAL_CURRENT * (1 - 2 * end)
                field[t, at, :] = field[t, at, :] + jnp.where(lane == j - t * TILE, sign, 0.0)

        return 0

    lax.fori_loop(1, count, one, 0)

    valid = (1 - nodata[...]).astype(jnp.float32)
    active = cond[...] * valid
    cells[0:rows, :] = active
    cells[rows : 2 * rows, :] = valid
    grounded = ground_mask[...].astype(jnp.float32) * ground_value[...]
    cells[2 * rows : 3 * rows, :] = grounded

    split_rows(field, pre, outer_rows(rows), tiles_hbm, tiles, tile_sems, parts, rows)
    apply_tiles(field, pre, [(r, parts, n) for n, r in enumerate(outer_rows(rows))], rows, chunks, 1)

    for rim, first, outermost in ((up_ref, 0, 0), (down_ref, rows - 2, rows - 1)):
        two = slice(first, first + 2)
        for t in range(cols // TILE):
            lanes = slice(t * TILE, (t + 1) * TILE)
            at = 2 * pairs + t * RIM
            rim[at : at + 2, :] = pre[t, two, :]
            rim[at + 2 : at + 4, :] = active[two, lanes]
            rim[at + 4 : at + 6, :] = valid[two, lanes]
            rim[at + 6 : at + 7, :] = grounded[outermost : outermost + 1, lanes]

    def selected(s, _):
        k = index[pairs + s]
        for end in range(2):
            i = index[pairs + slots + 2 * s + end]
            j = index[pairs + 3 * slots + 2 * s + end]
            t = lax.div(j, TILE)
            for rim, first, place in ((up_ref, 0, 0), (down_ref, rows - 2, 2)):

                @pl.when((i >= first) & (i < first + 2))
                def _():
                    rim[pl.ds(end * pairs + k, 1), :] = tiles[i - first + place, t, pl.ds(j - t * TILE, 1), :]

        return 0

    lax.fori_loop(1, count, selected, 0)


def inner_kernel(
    index, cells, field, parts, tiles_hbm, outer_pre, pre, second, image, tiles, inner_parts, sems, *, rows, cols, pairs, slots
):
    rest = range(2, rows - 2)
    for n, r in enumerate(rest):
        pltpu.make_async_copy(tiles_hbm.at[r], tiles.at[n], sems.at[n]).start()
    count = index[pairs + 5 * slots]
    chunks = (count + CHUNK - 1) // CHUNK
    active, valid, grounded = (cells[n * rows : (n + 1) * rows, :] for n in range(3))
    zero = jnp.zeros((1, cols), jnp.float32)
    weights = weights_of(active, valid, grounded, stacked(active, zero, zero), stacked(valid, zero, zero))

    keep_rows(outer_pre, pre, outer_rows(rows), rows, chunks)
    split_rows(field, pre, rest, tiles_hbm, tiles, sems, inner_parts, rows)
    inner = [(r, inner_parts, n) for n, r in enumerate(rest)]
    apply_tiles(field, pre, inner, rows, chunks, 1)

    def one(s, _):
        at = pl.ds(s * rows, rows)
        z = load(pre, at)
        store(image, at, operator(z, *stacked(z, zero, zero), weights))
        return 0

    lax.fori_loop(0, count, one, 0)
    apply_tiles(image, second, [(1, parts, 1), *inner, (rows - 2, parts, 2)], rows, chunks)


def middle_kernel(
    index,
    cells,
    field,
    pre,
    parts,
    above,
    below,
    tiles_above,
    tiles_below,
    inner_second,
    image,
    second,
    last,
    sums,
    outer,
    weights,
    rim_weights,
    kept_sem,
    *by_pair,
    rows,
    cols,
    pairs,
    slots,
):
    first_chunk = pl.ds(0, CHUNK * rows)
    kept = pltpu.make_async_copy(inner_second.at[:, first_chunk, :], second.at[:, first_chunk, :], kept_sem)
    kept.start()
    count = index[pairs + 5 * slots]
    chunks = (count + CHUNK - 1) // CHUNK
    active, valid, grounded = (cells[n * rows : (n + 1) * rows, :] for n in range(3))

    def told(rim, n):
        first = [2 * pairs + t * RIM + n for t in range(cols // TILE)]
        return jnp.concatenate([rim[i : i + 1, :] for i in first], axis=1)

    def own(x, i):
        return x[i : i + 1, :]

    def two(x, y):
        return jnp.concatenate([x, y], axis=0)

    active_a, active_b = (told(above, 2), told(above, 3)), (told(below, 2), told(below, 3))
    valid_a, valid_b = (told(above, 4), told(above, 5)), (told(below, 4), told(below, 5))
    all_weights = weights_of(
        active,
        valid,
        grounded,
        stacked(active, active_a[1], active_b[0]),
        stacked(valid, valid_a[1], valid_b[0]),
    )
    all_rim_weights = weights_of(
        two(active_a[1], active_b[0]),
        two(valid_a[1], valid_b[0]),
        two(told(above, 6), told(below, 6)),
        (two(active_a[0], own(active, rows - 1)), two(own(active, 0), active_b[1])),
        (two(valid_a[0], own(valid, rows - 1)), two(own(valid, 0), valid_b[1])),
    )
    for n in range(5):
        weights[n * rows : (n + 1) * rows, :] = all_weights[n]
        rim_weights[n * 8 : n * 8 + 2, :] = all_rim_weights[n]
    shared = jnp.concatenate([told(above, 0), told(above, 1), told(below, 0), told(below, 1)], axis=0)

    def near(s, _):
        k = index[pairs + s]
        store(outer, pl.ds(s * RIM, 4), shared)
        for end in range(2):
            i = index[pairs + slots + 2 * s + end]
            t = lax.div(index[pairs + 3 * slots + 2 * s + end], TILE)
            sign = FOCAL_CURRENT * (1 - 2 * end)
            for rim, first, place in ((above, -2, 0), (below, rows, 2)):

                @pl.when((i >= first) & (i < first + 2))
                def _():
                    at = pl.ds(s * RIM + i - first + place, 1)
                    outer[t, at, :] = outer[t, at, :] + sign * rim[pl.ds(end * pairs + k, 1), :]

        return 0

    store(outer, slice(0, 4), shared)
    lax.fori_loop(1, count, near, 0)

    def first_image(g, _):
        for s in [g * GROUP + n for n in range(GROUP)]:
            at = s * RIM
            z = load(pre, pl.ds(s * rows, rows))
            z_two = load(outer, pl.ds(at + 1, 2))
            w = [weights[n * rows : (n + 1) * rows, :] for n in range(5)]
            store(image, pl.ds(s * rows, rows), operator(z, *stacked(z, own(z_two, 0), own(z_two, 1)), w))
            w = [rim_weights[n * 8 : n * 8 + 2, :] for n in range(5)]
            up = two(load(outer, pl.ds(at, 1)), own(z, rows - 1))
            down = two(own(z, 0), load(outer, pl.ds(at + 3, 1)))
            store(outer, pl.ds(at + 4, 2), operator(z_two, up, down, w))
        return 0

    groups = (count + GROUP - 1) // GROUP
    lax.fori_loop(0, groups, first_image, 0)

    kept.wait()
    keep_rows(inner_second, second, range(1, rows - 1), rows, chunks, 1)

    def outer_tiles(c, _):
        for tiles, row in ((tiles_above, 4), (tiles_below, 5)):
            at = pl.ds(c * (CHUNK * RIM) + row, CHUNK, stride=RIM)
            to = pl.ds(c * (CHUNK * RIM) + row + 2, CHUNK, stride=RIM)
            for t in range(cols // TILE):
                pair = jnp.concatenate(cut(unpacked(tiles, t, cols // TILE)), axis=1)
                outer.at[t][to, :] = times_tile(outer.at[t][at, :], pair)
        for r, n in ((0, 0), (rows - 1, 3)):
            at = pl.ds(c * (CHUNK * rows) + r, CHUNK, stride=rows)
            for t in range(cols // TILE):
                second.at[t][at, :] = times_tile(image.at[t][at, :], parts[n, t])
        return 0

    lax.fori_loop(0, chunks, outer_tiles, 0)

    def folded(x):
        acc = x[:, 0:TILE]
        for t in range(1, cols // TILE):
            acc = acc + x[:, t * TILE : (t + 1) * TILE]
        return jnp.sum(acc, axis=0, keepdims=True)

    def four(s):
        at = pl.ds(s * rows, rows)
        w = [weights[n * rows : (n + 1) * rows, :] for n in range(5)]
        u, u_two = load(second, at), load(outer, pl.ds(s * RIM + 6, 2))
        v = operator(u, *stacked(u, own(u_two, 0), own(u_two, 1)), w)
        store(last, at, v)
        z, i = load(pre, at), load(image, at)
        return folded(load(field, at) * z), folded(z * i), folded(i * u), folded(u * v)

    def group(g, shared):
        members = [g * GROUP + n for n in range(GROUP)]
        sums_of = [four(s) for s in members]
        if shared:
            for part, x in zip(by_pair, sums_of[0]):
                part[...] = jnp.broadcast_to(x, part.shape)
        for s, four_sums in zip(members, sums_of):
            for part, x in zip(by_pair, four_sums):
                part[pl.ds(index[pairs + s], 1), :] = x

    def later(g, _):
        group(g, False)
        return 0

    group(0, True)
    lax.fori_loop(1, groups, later, 0)
    for n in range(2):
        both = jnp.concatenate([by_pair[2 * n + m][0:pairs, :] for m in range(2)], axis=0)
        sums[n : n + 1, :] = jnp.sum(both.T, axis=0, keepdims=True)


def finish_kernel(
    index,
    everyone,
    field,
    pre,
    image,
    second,
    last,
    solution_hbm,
    residual_hbm,
    first_c,
    second_c,
    solution,
    residual,
    solution_sems,
    residual_sems,
    *,
    rows,
    cols,
    pairs,
    block,
):
    total = jnp.sum(everyone[...], axis=0)
    ab, cd = total[0:1, :], total[1:2, :]
    gamma, delta = ab[:, :pairs], ab[:, pairs:]
    eta, theta = cd[:, :pairs], cd[:, pairs:]
    alpha = gamma / delta
    gamma_next = alpha * alpha * eta - gamma
    beta = 1.0 + gamma_next / gamma
    curvature = beta * beta * delta - 2.0 * beta * alpha * eta + alpha * alpha * theta
    step_next = gamma_next / curvature
    both = jnp.concatenate([alpha + step_next * beta, alpha * step_next], axis=1)
    spread = jnp.broadcast_to(both, (2 * pairs, 2 * pairs)).T
    first_c[...] = spread[:pairs, :]
    second_c[...] = spread[pairs:, :]

    def copies(n):
        at = pl.ds(n * block, block)
        return (
            pltpu.make_async_copy(solution.at[at], solution_hbm.at[at], solution_sems.at[n]),
            pltpu.make_async_copy(residual.at[at], residual_hbm.at[at], residual_sems.at[n]),
        )

    def one(n, _):
        for p in range(block):
            k = n * block + p
            at = pl.ds(pl.multiple_of(index[k] * rows, 8), rows)
            a = jnp.broadcast_to(first_c[pl.ds(k, 1), :], (rows, TILE))
            b = jnp.broadcast_to(second_c[pl.ds(k, 1), :], (rows, TILE))
            for t in range(cols // TILE):
                lanes = slice(t * TILE, (t + 1) * TILE)
                solution[k, :, lanes] = a * pre[t, at, :] - b * second[t, at, :]
                residual[k, :, lanes] = field[t, at, :] - a * image[t, at, :] + b * last[t, at, :]
        for copy in copies(n):
            copy.start()
        return 0

    lax.fori_loop(0, pairs // block, one, 0)

    def arrived(n, _):
        for copy in copies(n):
            copy.wait()
        return 0

    lax.fori_loop(0, pairs // block, arrived, 0)


def smem():
    return pl.BlockSpec(memory_space=pltpu.SMEM)


def vmem():
    return pl.BlockSpec(memory_space=pltpu.VMEM)


def hbm():
    return pl.BlockSpec(memory_space=pltpu.HBM)


def neighbours(up, down):
    count = lax.axis_size("space")
    ends = count - 1
    above = lax.ppermute(down, "space", [(i, (i + 1) % count) for i in range(ends)])
    below = lax.ppermute(up, "space", [((i + 1) % count, i) for i in range(ends)])
    return above, below


def on_device(conductance, nodata, ground_mask, ground_value, source_mask, source_current, tile_inverse, focal_cells):
    rows, cols = conductance.shape
    pairs = focal_cells.shape[0]
    slots = -(-(pairs + 1) // CHUNK) * CHUNK
    devices = lax.axis_size("space")
    f32 = jnp.float32
    sizes = dict(rows=rows, cols=cols, pairs=pairs, slots=slots)
    strip, fields, rim = (rows, cols), (cols // TILE, slots * rows, TILE), (2 * pairs + cols // TILE * RIM, TILE)
    per_row = tile_inverse.shape[1:]
    limit = pltpu.CompilerParams(vmem_limit_bytes=24 * MIB)
    base_row = (lax.axis_index("space") * rows).astype(jnp.int32).reshape(1)

    def shaped(shape, dtype=f32):
        return jax.ShapeDtypeStruct(shape, dtype)

    up, down = pl.pallas_call(
        functools.partial(pack_kernel, rows=rows),
        in_specs=[hbm()],
        out_specs=[vmem()] * 2,
        out_shape=[shaped((cols // TILE * (HALF + 1), TILE))] * 2,
        scratch_shapes=[pltpu.VMEM((2, *per_row), f32), pltpu.SemaphoreType.DMA((2,))],
        compiler_params=limit,
        name="pack",
    )(pltpu.with_memory_space_constraint(tile_inverse, pltpu.HBM))
    tiles_above, tiles_below = neighbours(up, down)
    field, pre, index, parts, cells, up, down = pl.pallas_call(
        functools.partial(start_kernel, **sizes),
        in_specs=[smem(), *[hbm()] * 8],
        out_specs=[vmem(), vmem(), smem(), *[vmem()] * 4],
        out_shape=[
            shaped(fields),
            shaped(fields),
            shaped((pairs + 5 * slots + 8,), jnp.int32),
            shaped((4, *per_row[:2], 2 * TILE), jnp.bfloat16),
            shaped((3 * rows, cols)),
            shaped(rim),
            shaped(rim),
        ],
        scratch_shapes=[
            pltpu.SMEM(focal_cells.shape[::-1], jnp.int32),
            pltpu.VMEM(strip, jnp.int32),
            pltpu.VMEM(strip, f32),
            pltpu.VMEM(strip, f32),
            pltpu.VMEM(strip, jnp.int32),
            pltpu.VMEM(strip, jnp.int32),
            pltpu.VMEM(strip, f32),
            pltpu.VMEM((4, *per_row), f32),
            pltpu.SemaphoreType.DMA,
            pltpu.SemaphoreType.DMA((6,)),
            pltpu.SemaphoreType.DMA((4,)),
        ],
        compiler_params=limit,
        name="start",
    )(
        base_row,
        *(
            pltpu.with_memory_space_constraint(x, pltpu.HBM)
            for x in (
                focal_cells.T,
                source_mask,
                source_current,
                conductance,
                nodata,
                ground_mask,
                ground_value,
                tile_inverse,
            )
        ),
    )
    above, below = neighbours(up, down)

    pre, inner_second = pl.pallas_call(
        functools.partial(inner_kernel, **sizes),
        in_specs=[smem(), *[vmem()] * 3, hbm(), vmem()],
        out_specs=[vmem()] * 2,
        out_shape=[shaped(fields)] * 2,
        scratch_shapes=[
            pltpu.VMEM(fields, f32),
            pltpu.VMEM((rows - 4, *per_row), f32),
            pltpu.VMEM((rows - 4, *per_row[:2], 2 * TILE), jnp.bfloat16),
            pltpu.SemaphoreType.DMA((rows - 4,)),
        ],
        compiler_params=limit,
        name="inner",
    )(index, cells, field, parts, pltpu.with_memory_space_constraint(tile_inverse, pltpu.HBM), pre)

    image, second, last, sums = pl.pallas_call(
        functools.partial(middle_kernel, **sizes),
        in_specs=[smem(), *[vmem()] * 9],
        out_specs=[vmem()] * 4,
        out_shape=[*[shaped(fields)] * 3, shaped((2, 2 * pairs))],
        scratch_shapes=[
            pltpu.VMEM((cols // TILE, slots * RIM, TILE), f32),
            pltpu.VMEM((5 * rows, cols), f32),
            pltpu.VMEM((5 * 8, cols), f32),
            pltpu.SemaphoreType.DMA,
            *[pltpu.VMEM((pairs + 8, TILE), f32)] * 4,
        ],
        compiler_params=limit,
        name="middle",
    )(index, cells, field, pre, parts, above, below, tiles_above, tiles_below, inner_second)
    copies = jnp.broadcast_to(sums, (devices, *sums.shape))
    everyone = lax.all_to_all(copies, "space", split_axis=0, concat_axis=0, tiled=True)

    block = 8
    out = (pairs, rows, cols)
    return pl.pallas_call(
        functools.partial(finish_kernel, rows=rows, cols=cols, pairs=pairs, block=block),
        in_specs=[smem(), *[vmem()] * 6],
        out_specs=[hbm()] * 2,
        out_shape=[shaped(out)] * 2,
        scratch_shapes=[
            pltpu.VMEM((pairs, TILE), f32),
            pltpu.VMEM((pairs, TILE), f32),
            pltpu.VMEM(out, f32),
            pltpu.VMEM(out, f32),
            pltpu.SemaphoreType.DMA((pairs // block,)),
            pltpu.SemaphoreType.DMA((pairs // block,)),
        ],
        compiler_params=limit,
        name="finish",
    )(index, everyone, field, pre, image, second, last)


def solution(mesh):
    cells = P(("groups", "space"), None)
    return jax.shard_map(
        on_device,
        mesh=mesh,
        in_specs=(*[cells] * 6, P(("groups", "space"), None, None, None), P(("groups", "rhs"), None)),
        out_specs=(P("rhs", ("groups", "space"), None), P("rhs", ("groups", "space"), None)),
        check_vma=False,
    )
```

```python
import functools

import jax
import jax.numpy as jnp
from jax import lax
from jax.experimental import pallas as pl
from jax.experimental.pallas import tpu as pltpu
from jax.sharding import PartitionSpec as P


LEAKAGE = 0.05
FOCAL_CURRENT = 16.0
TILE = 128
HALF = TILE // 2
CHUNK = 16
GROUP = 4
MIB = 1024 * 1024

RIM = 8


def cut(x):
    high = x.astype(jnp.bfloat16)
    return high, (x - high.astype(jnp.float32)).astype(jnp.bfloat16)


def load(field, at):
    return jnp.concatenate([field[t, at, :] for t in range(field.shape[0])], axis=1)


def store(field, at, x):
    for t in range(field.shape[0]):
        field[t, at, :] = x[:, t * TILE : (t + 1) * TILE]


def times_tile(x, pair):
    x_high, x_low = cut(x)
    y = jnp.dot(jnp.concatenate([x_high, x_low], axis=0), pair, preferred_element_type=jnp.float32)
    n = x.shape[0]
    return (y[:n, :TILE] + y[n:, TILE:]) + (y[n:, :TILE] + y[:n, TILE:])


def apply_tiles(src, dst, which, rows, chunks, first=0):
    def one(c, _):
        for r, parts, n in which:
            at = pl.ds(c * (CHUNK * rows) + r, CHUNK, stride=rows)
            for t in range(src.shape[0]):
                dst.at[t][at, :] = times_tile(src.at[t][at, :], parts[n, t])
        return 0

    lax.fori_loop(first, chunks, one, 0)


def keep_rows(src, dst, which, rows, chunks, first=0):
    def one(c, _):
        for r in which:
            at = pl.ds(c * (CHUNK * rows) + r, CHUNK, stride=rows)
            for t in range(src.shape[0]):
                dst.at[t][at, :] = src.at[t][at, :]
        return 0

    lax.fori_loop(first, chunks, one, 0)


def split_rows(src, dst, which, tiles, parts, rows, copies=None):
    for n, r in enumerate(which):
        if copies is not None:
            copies[n].wait()
        at = pl.ds(r, CHUNK, stride=rows)
        for t in range(src.shape[0]):
            pair = jnp.concatenate(cut(tiles[n, t]), axis=1)
            parts[n, t] = pair
            dst.at[t][at, :] = times_tile(src.at[t][at, :], pair)


def outer_rows(rows):
    return (0, 1, rows - 2, rows - 1)


def beside(x):
    cols = x.shape[1]
    return pltpu.roll(x, 1, 1), pltpu.roll(x, cols - 1, 1)


def stacked(x, above, below):
    rows = x.shape[0]
    row = lax.broadcasted_iota(jnp.int32, x.shape, 0)
    up = jnp.where(row == 0, above, pltpu.roll(x, 1, 0))
    down = jnp.where(row == rows - 1, below, pltpu.roll(x, rows - 1, 0))
    return up, down


def operator(x, up, down, weights):
    left, right = beside(x)
    diag, north, south, west, east = weights
    return diag * x - north * up - south * down - west * left - east * right


def weights_of(active, valid, grounded, active_beside, valid_beside):
    cols = active.shape[1]
    lane = lax.broadcasted_iota(jnp.int32, active.shape, 1)
    inside = (None, None, lane > 0, lane < cols - 1)
    edges = []
    for g, v, keep in zip((*active_beside, *beside(active)), (*valid_beside, *beside(valid)), inside):
        edge = 0.5 * (active + g) * valid * v
        edges.append(edge if keep is None else jnp.where(keep, edge, 0.0))
    north, south, west, east = edges
    diag = valid * (LEAKAGE + grounded) + (1.0 - valid) + north + south + west + east
    return diag, north, south, west, east


def below_diagonal():
    row = lax.broadcasted_iota(jnp.int32, (HALF, TILE), 0)
    lane = lax.broadcasted_iota(jnp.int32, (HALF, TILE), 1)
    return lane < row, lane == row + HALF


def pack_kernel(tiles_hbm, up_ref, down_ref, tiles, sems, *, rows):
    copies = [pltpu.make_async_copy(tiles_hbm.at[r], tiles.at[n], sems.at[n]) for n, r in enumerate((0, rows - 1))]
    for copy in copies:
        copy.start()
    moved, diagonal = below_diagonal()
    count = tiles.shape[1]
    for n, packed in enumerate((up_ref, down_ref)):
        copies[n].wait()
        for t in range(count):
            upper, lower = tiles[n, t, :HALF, :], tiles[n, t, HALF:, :]
            packed[t * HALF : (t + 1) * HALF, :] = jnp.where(moved, pltpu.roll(lower, HALF, 1), upper)
            at = count * HALF + t
            packed[at : at + 1, :] = jnp.sum(jnp.where(diagonal, lower, 0.0), axis=0, keepdims=True)


def unpacked(packed, t, count):
    x = packed[t * HALF : (t + 1) * HALF, :]
    diagonal = packed[count * HALF + t : count * HALF + t + 1, :]
    moved, _ = below_diagonal()
    top = jnp.where(moved, 0.0, x)
    bottom = pltpu.roll(jnp.where(moved, x, 0.0), HALF, 1)
    half = jnp.concatenate([top, bottom], axis=0)
    row = lax.broadcasted_iota(jnp.int32, (TILE, TILE), 0)
    lane = lax.broadcasted_iota(jnp.int32, (TILE, TILE), 1)
    return jnp.where(row == lane, jnp.where(row < HALF, half, diagonal), half + half.T)


def start_kernel(
    where,
    focal_hbm,
    mask_hbm,
    current_hbm,
    cond_hbm,
    nodata_hbm,
    ground_mask_hbm,
    ground_value_hbm,
    tiles_hbm,
    field,
    pre,
    index,
    parts,
    cells,
    inner_tiles,
    up_ref,
    down_ref,
    focal,
    mask,
    current,
    cond,
    nodata,
    ground_mask,
    ground_value,
    tiles,
    focal_sem,
    small_sems,
    tile_sems,
    inner_sem,
    *,
    rows,
    cols,
    pairs,
    slots,
):
    cells_of_pairs = pltpu.make_async_copy(focal_hbm, focal, focal_sem)
    cells_of_pairs.start()
    arrivals = [
        pltpu.make_async_copy(src, dst, small_sems.at[n])
        for n, (src, dst) in enumerate(
            [
                (mask_hbm, mask),
                (current_hbm, current),
                (cond_hbm, cond),
                (nodata_hbm, nodata),
                (ground_mask_hbm, ground_mask),
                (ground_value_hbm, ground_value),
            ]
        )
    ]
    for copy in arrivals:
        copy.start()
    tile_copies = [
        pltpu.make_async_copy(tiles_hbm.at[r], tiles.at[n], tile_sems.at[n]) for n, r in enumerate(outer_rows(rows))
    ]
    inner_copy = pltpu.make_async_copy(tiles_hbm.at[2 : rows - 2], inner_tiles, inner_sem)
    for copy in (*tile_copies, inner_copy):
        copy.start()

    base_row = where[0]
    cells_of_pairs.wait()

    def is_near(cell):
        return (cell >= (base_row - 2) * cols) & (cell < (base_row + rows + 2) * cols)

    def listed(k, s):
        near = is_near(focal[0, k]) | is_near(focal[1, k])
        index[k] = jnp.where(near, s, 0)
        index[pairs + s] = k
        return s + near.astype(jnp.int32)

    index[pairs] = pairs
    count = lax.fori_loop(0, pairs, listed, jnp.int32(1), unroll=8)
    index[pairs + 5 * slots] = count
    for n in range(GROUP):
        index[pairs + count + n] = pairs
    chunks = (count + CHUNK - 1) // CHUNK

    for copy in arrivals:
        copy.wait()
    background = mask[...].astype(jnp.float32) * current[...]
    store(field, slice(0, rows), background)
    lane = lax.broadcasted_iota(jnp.int32, (1, TILE), 1)

    def one(s, _):
        store(field, pl.ds(s * rows, rows), background)
        for end in range(2):
            cell = focal[end, index[pairs + s]]
            i = lax.div(cell, cols)
            j = cell - i * cols
            i = i - base_row
            index[pairs + slots + 2 * s + end] = i
            index[pairs + 3 * slots + 2 * s + end] = j

            @pl.when((i >= 0) & (i < rows))
            def _():
                t = lax.div(j, TILE)
                at = pl.ds(s * rows + i, 1)
                sign = FOCAL_CURRENT * (1 - 2 * end)
                field[t, at, :] = field[t, at, :] + jnp.where(lane == j - t * TILE, sign, 0.0)

        return 0

    lax.fori_loop(1, count, one, 0)

    valid = (1 - nodata[...]).astype(jnp.float32)
    active = cond[...] * valid
    cells[0:rows, :] = active
    cells[rows : 2 * rows, :] = valid
    grounded = ground_mask[...].astype(jnp.float32) * ground_value[...]
    cells[2 * rows : 3 * rows, :] = grounded

    split_rows(field, pre, outer_rows(rows), tiles, parts, rows, tile_copies)
    apply_tiles(field, pre, [(r, parts, n) for n, r in enumerate(outer_rows(rows))], rows, chunks, 1)

    for rim, first, outermost in ((up_ref, 0, 0), (down_ref, rows - 2, rows - 1)):
        two = slice(first, first + 2)
        for t in range(cols // TILE):
            lanes = slice(t * TILE, (t + 1) * TILE)
            at = 2 * pairs + t * RIM
            rim[at : at + 2, :] = pre[t, two, :]
            rim[at + 2 : at + 4, :] = active[two, lanes]
            rim[at + 4 : at + 6, :] = valid[two, lanes]
            rim[at + 6 : at + 7, :] = grounded[outermost : outermost + 1, lanes]

    def selected(s, _):
        k = index[pairs + s]
        for end in range(2):
            i = index[pairs + slots + 2 * s + end]
            j = index[pairs + 3 * slots + 2 * s + end]
            t = lax.div(j, TILE)
            for rim, first, place in ((up_ref, 0, 0), (down_ref, rows - 2, 2)):

                @pl.when((i >= first) & (i < first + 2))
                def _():
                    rim[pl.ds(end * pairs + k, 1), :] = tiles[i - first + place, t, pl.ds(j - t * TILE, 1), :]

        return 0

    lax.fori_loop(1, count, selected, 0)
    inner_copy.wait()


def inner_kernel(
    index, cells, field, parts, tiles, outer_pre, pre, second, image, inner_parts, *, rows, cols, pairs, slots
):
    rest = range(2, rows - 2)
    count = index[pairs + 5 * slots]
    chunks = (count + CHUNK - 1) // CHUNK
    active, valid, grounded = (cells[n * rows : (n + 1) * rows, :] for n in range(3))
    zero = jnp.zeros((1, cols), jnp.float32)
    weights = weights_of(active, valid, grounded, stacked(active, zero, zero), stacked(valid, zero, zero))

    keep_rows(outer_pre, pre, outer_rows(rows), rows, chunks)
    split_rows(field, pre, rest, tiles, inner_parts, rows)
    inner = [(r, inner_parts, n) for n, r in enumerate(rest)]
    apply_tiles(field, pre, inner, rows, chunks, 1)

    def one(s, _):
        at = pl.ds(s * rows, rows)
        z = load(pre, at)
        store(image, at, operator(z, *stacked(z, zero, zero), weights))
        return 0

    lax.fori_loop(0, count, one, 0)
    apply_tiles(image, second, [(1, parts, 1), *inner, (rows - 2, parts, 2)], rows, chunks)


def middle_kernel(
    index,
    cells,
    field,
    pre,
    parts,
    above,
    below,
    tiles_above,
    tiles_below,
    inner_second,
    image,
    second,
    last,
    sums,
    outer,
    weights,
    rim_weights,
    kept_sem,
    *by_pair,
    rows,
    cols,
    pairs,
    slots,
):
    first_chunk = pl.ds(0, CHUNK * rows)
    kept = pltpu.make_async_copy(inner_second.at[:, first_chunk, :], second.at[:, first_chunk, :], kept_sem)
    kept.start()
    count = index[pairs + 5 * slots]
    chunks = (count + CHUNK - 1) // CHUNK
    active, valid, grounded = (cells[n * rows : (n + 1) * rows, :] for n in range(3))

    def told(rim, n):
        first = [2 * pairs + t * RIM + n for t in range(cols // TILE)]
        return jnp.concatenate([rim[i : i + 1, :] for i in first], axis=1)

    def own(x, i):
        return x[i : i + 1, :]

    def two(x, y):
        return jnp.concatenate([x, y], axis=0)

    active_a, active_b = (told(above, 2), told(above, 3)), (told(below, 2), told(below, 3))
    valid_a, valid_b = (told(above, 4), told(above, 5)), (told(below, 4), told(below, 5))
    all_weights = weights_of(
        active,
        valid,
        grounded,
        stacked(active, active_a[1], active_b[0]),
        stacked(valid, valid_a[1], valid_b[0]),
    )
    all_rim_weights = weights_of(
        two(active_a[1], active_b[0]),
        two(valid_a[1], valid_b[0]),
        two(told(above, 6), told(below, 6)),
        (two(active_a[0], own(active, rows - 1)), two(own(active, 0), active_b[1])),
        (two(valid_a[0], own(valid, rows - 1)), two(own(valid, 0), valid_b[1])),
    )
    for n in range(5):
        weights[n * rows : (n + 1) * rows, :] = all_weights[n]
        rim_weights[n * 8 : n * 8 + 2, :] = all_rim_weights[n]
    shared = jnp.concatenate([told(above, 0), told(above, 1), told(below, 0), told(below, 1)], axis=0)

    def near(s, _):
        k = index[pairs + s]
        store(outer, pl.ds(s * RIM, 4), shared)
        for end in range(2):
            i = index[pairs + slots + 2 * s + end]
            t = lax.div(index[pairs + 3 * slots + 2 * s + end], TILE)
            sign = FOCAL_CURRENT * (1 - 2 * end)
            for rim, first, place in ((above, -2, 0), (below, rows, 2)):

                @pl.when((i >= first) & (i < first + 2))
                def _():
                    at = pl.ds(s * RIM + i - first + place, 1)
                    outer[t, at, :] = outer[t, at, :] + sign * rim[pl.ds(end * pairs + k, 1), :]

        return 0

    store(outer, slice(0, 4), shared)
    lax.fori_loop(1, count, near, 0)

    def first_image(g, _):
        for s in [g * GROUP + n for n in range(GROUP)]:
            at = s * RIM
            z = load(pre, pl.ds(s * rows, rows))
            z_two = load(outer, pl.ds(at + 1, 2))
            w = [weights[n * rows : (n + 1) * rows, :] for n in range(5)]
            store(image, pl.ds(s * rows, rows), operator(z, *stacked(z, own(z_two, 0), own(z_two, 1)), w))
            w = [rim_weights[n * 8 : n * 8 + 2, :] for n in range(5)]
            up = two(load(outer, pl.ds(at, 1)), own(z, rows - 1))
            down = two(own(z, 0), load(outer, pl.ds(at + 3, 1)))
            store(outer, pl.ds(at + 4, 2), operator(z_two, up, down, w))
        return 0

    groups = (count + GROUP - 1) // GROUP
    lax.fori_loop(0, groups, first_image, 0)

    kept.wait()
    keep_rows(inner_second, second, range(1, rows - 1), rows, chunks, 1)

    def outer_tiles(c, _):
        for tiles, row in ((tiles_above, 4), (tiles_below, 5)):
            at = pl.ds(c * (CHUNK * RIM) + row, CHUNK, stride=RIM)
            to = pl.ds(c * (CHUNK * RIM) + row + 2, CHUNK, stride=RIM)
            for t in range(cols // TILE):
                pair = jnp.concatenate(cut(unpacked(tiles, t, cols // TILE)), axis=1)
                outer.at[t][to, :] = times_tile(outer.at[t][at, :], pair)
        for r, n in ((0, 0), (rows - 1, 3)):
            at = pl.ds(c * (CHUNK * rows) + r, CHUNK, stride=rows)
            for t in range(cols // TILE):
                second.at[t][at, :] = times_tile(image.at[t][at, :], parts[n, t])
        return 0

    lax.fori_loop(0, chunks, outer_tiles, 0)

    def folded(x):
        acc = x[:, 0:TILE]
        for t in range(1, cols // TILE):
            acc = acc + x[:, t * TILE : (t + 1) * TILE]
        return jnp.sum(acc, axis=0, keepdims=True)

    def four(s):
        at = pl.ds(s * rows, rows)
        w = [weights[n * rows : (n + 1) * rows, :] for n in range(5)]
        u, u_two = load(second, at), load(outer, pl.ds(s * RIM + 6, 2))
        v = operator(u, *stacked(u, own(u_two, 0), own(u_two, 1)), w)
        store(last, at, v)
        z, i = load(pre, at), load(image, at)
        return folded(load(field, at) * z), folded(z * i), folded(i * u), folded(u * v)

    def group(g, shared):
        members = [g * GROUP + n for n in range(GROUP)]
        sums_of = [four(s) for s in members]
        if shared:
            for part, x in zip(by_pair, sums_of[0]):
                part[...] = jnp.broadcast_to(x, part.shape)
        for s, four_sums in zip(members, sums_of):
            for part, x in zip(by_pair, four_sums):
                part[pl.ds(index[pairs + s], 1), :] = x

    def later(g, _):
        group(g, False)
        return 0

    group(0, True)
    lax.fori_loop(1, groups, later, 0)
    for n in range(2):
        both = jnp.concatenate([by_pair[2 * n + m][0:pairs, :] for m in range(2)], axis=0)
        sums[n : n + 1, :] = jnp.sum(both.T, axis=0, keepdims=True)


def finish_kernel(
    index,
    everyone,
    field,
    pre,
    image,
    second,
    last,
    solution_hbm,
    residual_hbm,
    first_c,
    second_c,
    solution,
    residual,
    solution_sems,
    residual_sems,
    *,
    rows,
    cols,
    pairs,
    block,
):
    total = jnp.sum(everyone[...], axis=0)
    ab, cd = total[0:1, :], total[1:2, :]
    gamma, delta = ab[:, :pairs], ab[:, pairs:]
    eta, theta = cd[:, :pairs], cd[:, pairs:]
    alpha = gamma / delta
    gamma_next = alpha * alpha * eta - gamma
    beta = 1.0 + gamma_next / gamma
    curvature = beta * beta * delta - 2.0 * beta * alpha * eta + alpha * alpha * theta
    step_next = gamma_next / curvature
    both = jnp.concatenate([alpha + step_next * beta, alpha * step_next], axis=1)
    spread = jnp.broadcast_to(both, (2 * pairs, 2 * pairs)).T
    first_c[...] = spread[:pairs, :]
    second_c[...] = spread[pairs:, :]

    def copies(n):
        at = pl.ds(n * block, block)
        return (
            pltpu.make_async_copy(solution.at[at], solution_hbm.at[at], solution_sems.at[n]),
            pltpu.make_async_copy(residual.at[at], residual_hbm.at[at], residual_sems.at[n]),
        )

    def one(n, _):
        for p in range(block):
            k = n * block + p
            at = pl.ds(pl.multiple_of(index[k] * rows, 8), rows)
            a = jnp.broadcast_to(first_c[pl.ds(k, 1), :], (rows, TILE))
            b = jnp.broadcast_to(second_c[pl.ds(k, 1), :], (rows, TILE))
            for t in range(cols // TILE):
                lanes = slice(t * TILE, (t + 1) * TILE)
                solution[k, :, lanes] = a * pre[t, at, :] - b * second[t, at, :]
                residual[k, :, lanes] = field[t, at, :] - a * image[t, at, :] + b * last[t, at, :]
        for copy in copies(n):
            copy.start()
        return 0

    lax.fori_loop(0, pairs // block, one, 0)

    def arrived(n, _):
        for copy in copies(n):
            copy.wait()
        return 0

    lax.fori_loop(0, pairs // block, arrived, 0)


def smem():
    return pl.BlockSpec(memory_space=pltpu.SMEM)


def vmem():
    return pl.BlockSpec(memory_space=pltpu.VMEM)


def hbm():
    return pl.BlockSpec(memory_space=pltpu.HBM)


def neighbours(up, down):
    count = lax.axis_size("space")
    ends = count - 1
    below = lax.ppermute(up, "space", [((i + 1) % count, i) for i in range(ends)])
    above = lax.ppermute(down, "space", [(i, (i + 1) % count) for i in range(ends)])
    return above, below


def on_device(conductance, nodata, ground_mask, ground_value, source_mask, source_current, tile_inverse, focal_cells):
    rows, cols = conductance.shape
    pairs = focal_cells.shape[0]
    slots = -(-(pairs + 1) // CHUNK) * CHUNK
    devices = lax.axis_size("space")
    f32 = jnp.float32
    sizes = dict(rows=rows, cols=cols, pairs=pairs, slots=slots)
    strip, fields, rim = (rows, cols), (cols // TILE, slots * rows, TILE), (2 * pairs + cols // TILE * RIM, TILE)
    per_row = tile_inverse.shape[1:]
    limit = pltpu.CompilerParams(vmem_limit_bytes=24 * MIB)
    base_row = (lax.axis_index("space") * rows).astype(jnp.int32).reshape(1)

    def shaped(shape, dtype=f32):
        return jax.ShapeDtypeStruct(shape, dtype)

    up, down = pl.pallas_call(
        functools.partial(pack_kernel, rows=rows),
        in_specs=[hbm()],
        out_specs=[vmem()] * 2,
        out_shape=[shaped((cols // TILE * (HALF + 1), TILE))] * 2,
        scratch_shapes=[pltpu.VMEM((2, *per_row), f32), pltpu.SemaphoreType.DMA((2,))],
        compiler_params=limit,
        name="pack",
    )(pltpu.with_memory_space_constraint(tile_inverse, pltpu.HBM))
    tiles_above, tiles_below = neighbours(up, down)
    field, pre, index, parts, cells, inner_tiles, up, down = pl.pallas_call(
        functools.partial(start_kernel, **sizes),
        in_specs=[smem(), *[hbm()] * 8],
        out_specs=[vmem(), vmem(), smem(), *[vmem()] * 5],
        out_shape=[
            shaped(fields),
            shaped(fields),
            shaped((pairs + 5 * slots + 8,), jnp.int32),
            shaped((4, *per_row[:2], 2 * TILE), jnp.bfloat16),
            shaped((3 * rows, cols)),
            shaped((rows - 4, *per_row)),
            shaped(rim),
            shaped(rim),
        ],
        scratch_shapes=[
            pltpu.SMEM(focal_cells.shape[::-1], jnp.int32),
            pltpu.VMEM(strip, jnp.int32),
            pltpu.VMEM(strip, f32),
            pltpu.VMEM(strip, f32),
            pltpu.VMEM(strip, jnp.int32),
            pltpu.VMEM(strip, jnp.int32),
            pltpu.VMEM(strip, f32),
            pltpu.VMEM((4, *per_row), f32),
            pltpu.SemaphoreType.DMA,
            pltpu.SemaphoreType.DMA((6,)),
            pltpu.SemaphoreType.DMA((4,)),
            pltpu.SemaphoreType.DMA,
        ],
        compiler_params=limit,
        name="start",
    )(
        base_row,
        *(
            pltpu.with_memory_space_constraint(x, pltpu.HBM)
            for x in (
                focal_cells.T,
                source_mask,
                source_current,
                conductance,
                nodata,
                ground_mask,
                ground_value,
                tile_inverse,
            )
        ),
    )
    above, below = neighbours(up, down)

    pre, inner_second = pl.pallas_call(
        functools.partial(inner_kernel, **sizes),
        in_specs=[smem(), *[vmem()] * 5],
        out_specs=[vmem()] * 2,
        out_shape=[shaped(fields)] * 2,
        scratch_shapes=[
            pltpu.VMEM(fields, f32),
            pltpu.VMEM((rows - 4, *per_row[:2], 2 * TILE), jnp.bfloat16),
        ],
        compiler_params=limit,
        name="inner",
    )(index, cells, field, parts, inner_tiles, pre)

    image, second, last, sums = pl.pallas_call(
        functools.partial(middle_kernel, **sizes),
        in_specs=[smem(), *[vmem()] * 9],
        out_specs=[vmem()] * 4,
        out_shape=[*[shaped(fields)] * 3, shaped((2, 2 * pairs))],
        scratch_shapes=[
            pltpu.VMEM((cols // TILE, slots * RIM, TILE), f32),
            pltpu.VMEM((5 * rows, cols), f32),
            pltpu.VMEM((5 * 8, cols), f32),
            pltpu.SemaphoreType.DMA,
            *[pltpu.VMEM((pairs + 8, TILE), f32)] * 4,
        ],
        compiler_params=limit,
        name="middle",
    )(index, cells, field, pre, parts, above, below, tiles_above, tiles_below, inner_second)
    copies = jnp.broadcast_to(sums, (devices, *sums.shape))
    everyone = lax.all_to_all(copies, "space", split_axis=0, concat_axis=0, tiled=True)

    block = 8
    out = (pairs, rows, cols)
    return pl.pallas_call(
        functools.partial(finish_kernel, rows=rows, cols=cols, pairs=pairs, block=block),
        in_specs=[smem(), *[vmem()] * 6],
        out_specs=[hbm()] * 2,
        out_shape=[shaped(out)] * 2,
        scratch_shapes=[
            pltpu.VMEM((pairs, TILE), f32),
            pltpu.VMEM((pairs, TILE), f32),
            pltpu.VMEM(out, f32),
            pltpu.VMEM(out, f32),
            pltpu.SemaphoreType.DMA((pairs // block,)),
            pltpu.SemaphoreType.DMA((pairs // block,)),
        ],
        compiler_params=limit,
        name="finish",
    )(index, everyone, field, pre, image, second, last)


def solution(mesh):
    cells = P(("groups", "space"), None)
    return jax.shard_map(
        on_device,
        mesh=mesh,
        in_specs=(*[cells] * 6, P(("groups", "space"), None, None, None), P(("groups", "rhs"), None)),
        out_specs=(P("rhs", ("groups", "space"), None), P("rhs", ("groups", "space"), None)),
        check_vma=False,
    )
```

```python
import functools

import jax
import jax.numpy as jnp
from jax import lax
from jax.experimental import pallas as pl
from jax.experimental.pallas import tpu as pltpu
from jax.sharding import PartitionSpec as P

LEAKAGE = 0.05
FOCAL_CURRENT = 16.0
TILE = 128
HALF = TILE // 2
CHUNK = 16
GROUP = 4
MIB = 1024 * 1024

RIM = 8


def cut(x):
    high = x.astype(jnp.bfloat16)
    return high, (x - high.astype(jnp.float32)).astype(jnp.bfloat16)


def load(field, at):
    return jnp.concatenate([field[t, at, :] for t in range(field.shape[0])], axis=1)


def store(field, at, x):
    for t in range(field.shape[0]):
        field[t, at, :] = x[:, t * TILE : (t + 1) * TILE]


def times_tile(x, pair):
    x_high, x_low = cut(x)
    y = jnp.dot(jnp.concatenate([x_high, x_low], axis=0), pair, preferred_element_type=jnp.float32)
    n = x.shape[0]
    return (y[:n, :TILE] + y[n:, TILE:]) + (y[n:, :TILE] + y[:n, TILE:])


def apply_tiles(src, dst, which, rows, chunks, first=0):
    def one(c, _):
        for r, parts, n in which:
            at = pl.ds(c * (CHUNK * rows) + r, CHUNK, stride=rows)
            for t in range(src.shape[0]):
                dst.at[t][at, :] = times_tile(src.at[t][at, :], parts[n, t])
        return 0

    lax.fori_loop(first, chunks, one, 0)


def keep_rows(src, dst, which, rows, chunks, first=0):
    def one(c, _):
        for r in which:
            at = pl.ds(c * (CHUNK * rows) + r, CHUNK, stride=rows)
            for t in range(src.shape[0]):
                dst.at[t][at, :] = src.at[t][at, :]
        return 0

    lax.fori_loop(first, chunks, one, 0)


def split_rows(src, dst, which, tiles, parts, rows, copies=None):
    for n, r in enumerate(which):
        if copies is not None:
            copies[n].wait()
        at = pl.ds(r, CHUNK, stride=rows)
        for t in range(src.shape[0]):
            pair = jnp.concatenate(cut(tiles[n, t]), axis=1)
            parts[n, t] = pair
            dst.at[t][at, :] = times_tile(src.at[t][at, :], pair)


def outer_rows(rows):
    return (0, 1, rows - 2, rows - 1)


def beside(x):
    cols = x.shape[1]
    return pltpu.roll(x, 1, 1), pltpu.roll(x, cols - 1, 1)


def stacked(x, above, below):
    rows = x.shape[0]
    row = lax.broadcasted_iota(jnp.int32, x.shape, 0)
    up = jnp.where(row == 0, above, pltpu.roll(x, 1, 0))
    down = jnp.where(row == rows - 1, below, pltpu.roll(x, rows - 1, 0))
    return up, down


def operator(x, up, down, weights):
    left, right = beside(x)
    diag, north, south, west, east = weights
    return diag * x - north * up - south * down - west * left - east * right


def weights_of(active, valid, grounded, active_beside, valid_beside):
    cols = active.shape[1]
    lane = lax.broadcasted_iota(jnp.int32, active.shape, 1)
    inside = (None, None, lane > 0, lane < cols - 1)
    edges = []
    for g, v, keep in zip((*active_beside, *beside(active)), (*valid_beside, *beside(valid)), inside):
        edge = 0.5 * (active + g) * valid * v
        edges.append(edge if keep is None else jnp.where(keep, edge, 0.0))
    north, south, west, east = edges
    diag = valid * (LEAKAGE + grounded) + (1.0 - valid) + north + south + west + east
    return diag, north, south, west, east


def below_diagonal():
    row = lax.broadcasted_iota(jnp.int32, (HALF, TILE), 0)
    lane = lax.broadcasted_iota(jnp.int32, (HALF, TILE), 1)
    return lane < row, lane == row + HALF


def pack(tiles, n, packed, first):
    moved, diagonal = below_diagonal()
    count = tiles.shape[1]
    for t in range(count):
        upper, lower = tiles[n, t, :HALF, :], tiles[n, t, HALF:, :]
        at = first + t * HALF
        packed[at : at + HALF, :] = jnp.where(moved, pltpu.roll(lower, HALF, 1), upper)
        at = first + count * HALF + t
        packed[at : at + 1, :] = jnp.sum(jnp.where(diagonal, lower, 0.0), axis=0, keepdims=True)


def unpacked(packed, first, t, count):
    x = packed[first + t * HALF : first + (t + 1) * HALF, :]
    at = first + count * HALF + t
    diagonal = packed[at : at + 1, :]
    moved, _ = below_diagonal()
    top = jnp.where(moved, 0.0, x)
    bottom = pltpu.roll(jnp.where(moved, x, 0.0), HALF, 1)
    half = jnp.concatenate([top, bottom], axis=0)
    row = lax.broadcasted_iota(jnp.int32, (TILE, TILE), 0)
    lane = lax.broadcasted_iota(jnp.int32, (TILE, TILE), 1)
    return jnp.where(row == lane, jnp.where(row < HALF, half, diagonal), half + half.T)


def start_kernel(
    where,
    focal_hbm,
    mask_hbm,
    current_hbm,
    cond_hbm,
    nodata_hbm,
    ground_mask_hbm,
    ground_value_hbm,
    tiles_hbm,
    field,
    pre,
    index,
    parts,
    cells,
    inner_tiles,
    up_ref,
    down_ref,
    focal,
    mask,
    current,
    cond,
    nodata,
    ground_mask,
    ground_value,
    tiles,
    focal_sem,
    small_sems,
    tile_sems,
    inner_sem,
    *,
    rows,
    cols,
    pairs,
    slots,
):
    cells_of_pairs = pltpu.make_async_copy(focal_hbm, focal, focal_sem)
    cells_of_pairs.start()
    arrivals = [
        pltpu.make_async_copy(src, dst, small_sems.at[n])
        for n, (src, dst) in enumerate(
            [
                (mask_hbm, mask),
                (current_hbm, current),
                (cond_hbm, cond),
                (nodata_hbm, nodata),
                (ground_mask_hbm, ground_mask),
                (ground_value_hbm, ground_value),
            ]
        )
    ]
    for copy in arrivals:
        copy.start()
    tile_copies = [
        pltpu.make_async_copy(tiles_hbm.at[r], tiles.at[n], tile_sems.at[n]) for n, r in enumerate(outer_rows(rows))
    ]
    inner_copy = pltpu.make_async_copy(tiles_hbm.at[2 : rows - 2], inner_tiles, inner_sem)
    for copy in (*tile_copies, inner_copy):
        copy.start()

    base_row = where[0]
    cells_of_pairs.wait()

    def is_near(cell):
        return (cell >= (base_row - 2) * cols) & (cell < (base_row + rows + 2) * cols)

    def listed(k, s):
        near = is_near(focal[0, k]) | is_near(focal[1, k])
        index[k] = jnp.where(near, s, 0)
        index[pairs + s] = k
        return s + near.astype(jnp.int32)

    index[pairs] = pairs
    count = lax.fori_loop(0, pairs, listed, jnp.int32(1), unroll=8)
    index[pairs + 5 * slots] = count
    for n in range(GROUP):
        index[pairs + count + n] = pairs
    chunks = (count + CHUNK - 1) // CHUNK

    for copy in arrivals:
        copy.wait()
    background = mask[...].astype(jnp.float32) * current[...]
    store(field, slice(0, rows), background)
    lane = lax.broadcasted_iota(jnp.int32, (1, TILE), 1)

    def one(s, _):
        store(field, pl.ds(s * rows, rows), background)
        for end in range(2):
            cell = focal[end, index[pairs + s]]
            i = lax.div(cell, cols)
            j = cell - i * cols
            i = i - base_row
            index[pairs + slots + 2 * s + end] = i
            index[pairs + 3 * slots + 2 * s + end] = j

            @pl.when((i >= 0) & (i < rows))
            def _():
                t = lax.div(j, TILE)
                at = pl.ds(s * rows + i, 1)
                sign = FOCAL_CURRENT * (1 - 2 * end)
                field[t, at, :] = field[t, at, :] + jnp.where(lane == j - t * TILE, sign, 0.0)

        return 0

    lax.fori_loop(1, count, one, 0)

    valid = (1 - nodata[...]).astype(jnp.float32)
    active = cond[...] * valid
    cells[0:rows, :] = active
    cells[rows : 2 * rows, :] = valid
    grounded = ground_mask[...].astype(jnp.float32) * ground_value[...]
    cells[2 * rows : 3 * rows, :] = grounded

    split_rows(field, pre, outer_rows(rows), tiles, parts, rows, tile_copies)
    apply_tiles(field, pre, [(r, parts, n) for n, r in enumerate(outer_rows(rows))], rows, chunks, 1)

    for rim, first, outermost in ((up_ref, 0, 0), (down_ref, rows - 2, rows - 1)):
        pack(tiles, 0 if first == 0 else 3, rim, 2 * pairs + cols // TILE * RIM)
        two = slice(first, first + 2)
        for t in range(cols // TILE):
            lanes = slice(t * TILE, (t + 1) * TILE)
            at = 2 * pairs + t * RIM
            rim[at : at + 2, :] = pre[t, two, :]
            rim[at + 2 : at + 4, :] = active[two, lanes]
            rim[at + 4 : at + 6, :] = valid[two, lanes]
            rim[at + 6 : at + 7, :] = grounded[outermost : outermost + 1, lanes]

    def selected(s, _):
        k = index[pairs + s]
        for end in range(2):
            i = index[pairs + slots + 2 * s + end]
            j = index[pairs + 3 * slots + 2 * s + end]
            t = lax.div(j, TILE)
            for rim, first, place in ((up_ref, 0, 0), (down_ref, rows - 2, 2)):

                @pl.when((i >= first) & (i < first + 2))
                def _():
                    rim[pl.ds(end * pairs + k, 1), :] = tiles[i - first + place, t, pl.ds(j - t * TILE, 1), :]

        return 0

    lax.fori_loop(1, count, selected, 0)
    inner_copy.wait()


def inner_kernel(
    index, cells, field, parts, tiles, outer_pre, pre, second, image, inner_parts, *, rows, cols, pairs, slots
):
    rest = range(2, rows - 2)
    count = index[pairs + 5 * slots]
    chunks = (count + CHUNK - 1) // CHUNK
    active, valid, grounded = (cells[n * rows : (n + 1) * rows, :] for n in range(3))
    zero = jnp.zeros((1, cols), jnp.float32)
    weights = weights_of(active, valid, grounded, stacked(active, zero, zero), stacked(valid, zero, zero))

    keep_rows(outer_pre, pre, outer_rows(rows), rows, chunks)
    split_rows(field, pre, rest, tiles, inner_parts, rows)
    inner = [(r, inner_parts, n) for n, r in enumerate(rest)]
    apply_tiles(field, pre, inner, rows, chunks, 1)

    def one(s, _):
        at = pl.ds(s * rows, rows)
        z = load(pre, at)
        store(image, at, operator(z, *stacked(z, zero, zero), weights))
        return 0

    lax.fori_loop(0, count, one, 0)
    apply_tiles(image, second, [(1, parts, 1), *inner, (rows - 2, parts, 2)], rows, chunks)


def middle_kernel(
    index,
    cells,
    field,
    pre,
    parts,
    above,
    below,
    inner_second,
    image,
    second,
    last,
    sums,
    outer,
    weights,
    rim_weights,
    kept_sem,
    *by_pair,
    rows,
    cols,
    pairs,
    slots,
):
    first_chunk = pl.ds(0, CHUNK * rows)
    kept = pltpu.make_async_copy(inner_second.at[:, first_chunk, :], second.at[:, first_chunk, :], kept_sem)
    kept.start()
    count = index[pairs + 5 * slots]
    chunks = (count + CHUNK - 1) // CHUNK
    active, valid, grounded = (cells[n * rows : (n + 1) * rows, :] for n in range(3))

    def told(rim, n):
        first = [2 * pairs + t * RIM + n for t in range(cols // TILE)]
        return jnp.concatenate([rim[i : i + 1, :] for i in first], axis=1)

    def own(x, i):
        return x[i : i + 1, :]

    def two(x, y):
        return jnp.concatenate([x, y], axis=0)

    active_a, active_b = (told(above, 2), told(above, 3)), (told(below, 2), told(below, 3))
    valid_a, valid_b = (told(above, 4), told(above, 5)), (told(below, 4), told(below, 5))
    all_weights = weights_of(
        active,
        valid,
        grounded,
        stacked(active, active_a[1], active_b[0]),
        stacked(valid, valid_a[1], valid_b[0]),
    )
    all_rim_weights = weights_of(
        two(active_a[1], active_b[0]),
        two(valid_a[1], valid_b[0]),
        two(told(above, 6), told(below, 6)),
        (two(active_a[0], own(active, rows - 1)), two(own(active, 0), active_b[1])),
        (two(valid_a[0], own(valid, rows - 1)), two(own(valid, 0), valid_b[1])),
    )
    for n in range(5):
        weights[n * rows : (n + 1) * rows, :] = all_weights[n]
        rim_weights[n * 8 : n * 8 + 2, :] = all_rim_weights[n]
    shared = jnp.concatenate([told(above, 0), told(above, 1), told(below, 0), told(below, 1)], axis=0)

    def near(s, _):
        k = index[pairs + s]
        store(outer, pl.ds(s * RIM, 4), shared)
        for end in range(2):
            i = index[pairs + slots + 2 * s + end]
            t = lax.div(index[pairs + 3 * slots + 2 * s + end], TILE)
            sign = FOCAL_CURRENT * (1 - 2 * end)
            for rim, first, place in ((above, -2, 0), (below, rows, 2)):

                @pl.when((i >= first) & (i < first + 2))
                def _():
                    at = pl.ds(s * RIM + i - first + place, 1)
                    outer[t, at, :] = outer[t, at, :] + sign * rim[pl.ds(end * pairs + k, 1), :]

        return 0

    store(outer, slice(0, 4), shared)
    lax.fori_loop(1, count, near, 0)

    def first_image(g, _):
        for s in [g * GROUP + n for n in range(GROUP)]:
            at = s * RIM
            z = load(pre, pl.ds(s * rows, rows))
            z_two = load(outer, pl.ds(at + 1, 2))
            w = [weights[n * rows : (n + 1) * rows, :] for n in range(5)]
            store(image, pl.ds(s * rows, rows), operator(z, *stacked(z, own(z_two, 0), own(z_two, 1)), w))
            w = [rim_weights[n * 8 : n * 8 + 2, :] for n in range(5)]
            up = two(load(outer, pl.ds(at, 1)), own(z, rows - 1))
            down = two(own(z, 0), load(outer, pl.ds(at + 3, 1)))
            store(outer, pl.ds(at + 4, 2), operator(z_two, up, down, w))
        return 0

    groups = (count + GROUP - 1) // GROUP
    lax.fori_loop(0, groups, first_image, 0)

    kept.wait()
    keep_rows(inner_second, second, range(1, rows - 1), rows, chunks, 1)

    def outer_tiles(c, _):
        for rim, row in ((above, 4), (below, 5)):
            at = pl.ds(c * (CHUNK * RIM) + row, CHUNK, stride=RIM)
            to = pl.ds(c * (CHUNK * RIM) + row + 2, CHUNK, stride=RIM)
            for t in range(cols // TILE):
                pair = jnp.concatenate(cut(unpacked(rim, 2 * pairs + cols // TILE * RIM, t, cols // TILE)), axis=1)
                outer.at[t][to, :] = times_tile(outer.at[t][at, :], pair)
        for r, n in ((0, 0), (rows - 1, 3)):
            at = pl.ds(c * (CHUNK * rows) + r, CHUNK, stride=rows)
            for t in range(cols // TILE):
                second.at[t][at, :] = times_tile(image.at[t][at, :], parts[n, t])
        return 0

    lax.fori_loop(0, chunks, outer_tiles, 0)

    def folded(x):
        acc = x[:, 0:TILE]
        for t in range(1, cols // TILE):
            acc = acc + x[:, t * TILE : (t + 1) * TILE]
        return jnp.sum(acc, axis=0, keepdims=True)

    def four(s):
        at = pl.ds(s * rows, rows)
        w = [weights[n * rows : (n + 1) * rows, :] for n in range(5)]
        u, u_two = load(second, at), load(outer, pl.ds(s * RIM + 6, 2))
        v = operator(u, *stacked(u, own(u_two, 0), own(u_two, 1)), w)
        store(last, at, v)
        z, i = load(pre, at), load(image, at)
        return folded(load(field, at) * z), folded(z * i), folded(i * u), folded(u * v)

    def group(g, shared):
        members = [g * GROUP + n for n in range(GROUP)]
        sums_of = [four(s) for s in members]
        if shared:
            for part, x in zip(by_pair, sums_of[0]):
                part[...] = jnp.broadcast_to(x, part.shape)
        for s, four_sums in zip(members, sums_of):
            for part, x in zip(by_pair, four_sums):
                part[pl.ds(index[pairs + s], 1), :] = x

    def later(g, _):
        group(g, False)
        return 0

    group(0, True)
    lax.fori_loop(1, groups, later, 0)
    for n in range(2):
        both = jnp.concatenate([by_pair[2 * n + m][0:pairs, :] for m in range(2)], axis=0)
        sums[n : n + 1, :] = jnp.sum(both.T, axis=0, keepdims=True)


def finish_kernel(
    index,
    everyone,
    field,
    pre,
    image,
    second,
    last,
    solution_hbm,
    residual_hbm,
    first_c,
    second_c,
    solution,
    residual,
    solution_sems,
    residual_sems,
    *,
    rows,
    cols,
    pairs,
    block,
):
    total = jnp.sum(everyone[...], axis=0)
    ab, cd = total[0:1, :], total[1:2, :]
    gamma, delta = ab[:, :pairs], ab[:, pairs:]
    eta, theta = cd[:, :pairs], cd[:, pairs:]
    alpha = gamma / delta
    gamma_next = alpha * alpha * eta - gamma
    beta = 1.0 + gamma_next / gamma
    curvature = beta * beta * delta - 2.0 * beta * alpha * eta + alpha * alpha * theta
    step_next = gamma_next / curvature
    both = jnp.concatenate([alpha + step_next * beta, alpha * step_next], axis=1)
    spread = jnp.broadcast_to(both, (2 * pairs, 2 * pairs)).T
    first_c[...] = spread[:pairs, :]
    second_c[...] = spread[pairs:, :]

    def copies(n):
        at = pl.ds(n * block, block)
        return (
            pltpu.make_async_copy(solution.at[at], solution_hbm.at[at], solution_sems.at[n]),
            pltpu.make_async_copy(residual.at[at], residual_hbm.at[at], residual_sems.at[n]),
        )

    def one(n, _):
        for p in range(block):
            k = n * block + p
            at = pl.ds(pl.multiple_of(index[k] * rows, 8), rows)
            a = jnp.broadcast_to(first_c[pl.ds(k, 1), :], (rows, TILE))
            b = jnp.broadcast_to(second_c[pl.ds(k, 1), :], (rows, TILE))
            for t in range(cols // TILE):
                lanes = slice(t * TILE, (t + 1) * TILE)
                solution[k, :, lanes] = a * pre[t, at, :] - b * second[t, at, :]
                residual[k, :, lanes] = field[t, at, :] - a * image[t, at, :] + b * last[t, at, :]
        for copy in copies(n):
            copy.start()
        return 0

    lax.fori_loop(0, pairs // block, one, 0)

    def arrived(n, _):
        for copy in copies(n):
            copy.wait()
        return 0

    lax.fori_loop(0, pairs // block, arrived, 0)


def smem():
    return pl.BlockSpec(memory_space=pltpu.SMEM)


def vmem():
    return pl.BlockSpec(memory_space=pltpu.VMEM)


def hbm():
    return pl.BlockSpec(memory_space=pltpu.HBM)


def neighbours(up, down):
    count = lax.axis_size("space")
    ends = count - 1
    with jax.named_scope("up"):
        below = lax.ppermute(up, "space", [((i + 1) % count, i) for i in range(ends)])
    with jax.named_scope("down"):
        above = lax.ppermute(down, "space", [(i, (i + 1) % count) for i in range(ends)])
    return above, below


def on_device(conductance, nodata, ground_mask, ground_value, source_mask, source_current, tile_inverse, focal_cells):
    rows, cols = conductance.shape
    pairs = focal_cells.shape[0]
    slots = -(-(pairs + 1) // CHUNK) * CHUNK
    devices = lax.axis_size("space")
    f32 = jnp.float32
    sizes = dict(rows=rows, cols=cols, pairs=pairs, slots=slots)
    strip, fields, rim = (rows, cols), (cols // TILE, slots * rows, TILE), (2 * pairs + cols // TILE * (RIM + HALF + 1), TILE)
    per_row = tile_inverse.shape[1:]
    limit = pltpu.CompilerParams(vmem_limit_bytes=24 * MIB)
    base_row = (lax.axis_index("space") * rows).astype(jnp.int32).reshape(1)

    def shaped(shape, dtype=f32):
        return jax.ShapeDtypeStruct(shape, dtype)

    field, pre, index, parts, cells, inner_tiles, up, down = pl.pallas_call(
        functools.partial(start_kernel, **sizes),
        in_specs=[smem(), *[hbm()] * 8],
        out_specs=[vmem(), vmem(), smem(), *[vmem()] * 5],
        out_shape=[
            shaped(fields),
            shaped(fields),
            shaped((pairs + 5 * slots + 8,), jnp.int32),
            shaped((4, *per_row[:2], 2 * TILE), jnp.bfloat16),
            shaped((3 * rows, cols)),
            shaped((rows - 4, *per_row)),
            shaped(rim),
            shaped(rim),
        ],
        scratch_shapes=[
            pltpu.SMEM(focal_cells.shape[::-1], jnp.int32),
            pltpu.VMEM(strip, jnp.int32),
            pltpu.VMEM(strip, f32),
            pltpu.VMEM(strip, f32),
            pltpu.VMEM(strip, jnp.int32),
            pltpu.VMEM(strip, jnp.int32),
            pltpu.VMEM(strip, f32),
            pltpu.VMEM((4, *per_row), f32),
            pltpu.SemaphoreType.DMA,
            pltpu.SemaphoreType.DMA((6,)),
            pltpu.SemaphoreType.DMA((4,)),
            pltpu.SemaphoreType.DMA,
        ],
        compiler_params=limit,
        name="start",
    )(
        base_row,
        *(
            pltpu.with_memory_space_constraint(x, pltpu.HBM)
            for x in (
                focal_cells.T,
                source_mask,
                source_current,
                conductance,
                nodata,
                ground_mask,
                ground_value,
                tile_inverse,
            )
        ),
    )
    above, below = neighbours(up, down)

    pre, inner_second = pl.pallas_call(
        functools.partial(inner_kernel, **sizes),
        in_specs=[smem(), *[vmem()] * 5],
        out_specs=[vmem()] * 2,
        out_shape=[shaped(fields)] * 2,
        scratch_shapes=[
            pltpu.VMEM(fields, f32),
            pltpu.VMEM((rows - 4, *per_row[:2], 2 * TILE), jnp.bfloat16),
        ],
        compiler_params=limit,
        name="inner",
    )(index, cells, field, parts, inner_tiles, pre)

    image, second, last, sums = pl.pallas_call(
        functools.partial(middle_kernel, **sizes),
        in_specs=[smem(), *[vmem()] * 7],
        out_specs=[vmem()] * 4,
        out_shape=[*[shaped(fields)] * 3, shaped((2, 2 * pairs))],
        scratch_shapes=[
            pltpu.VMEM((cols // TILE, slots * RIM, TILE), f32),
            pltpu.VMEM((5 * rows, cols), f32),
            pltpu.VMEM((5 * 8, cols), f32),
            pltpu.SemaphoreType.DMA,
            *[pltpu.VMEM((pairs + 8, TILE), f32)] * 4,
        ],
        compiler_params=limit,
        name="middle",
    )(index, cells, field, pre, parts, above, below, inner_second)
    copies = jnp.broadcast_to(sums, (devices, *sums.shape))
    everyone = lax.all_to_all(copies, "space", split_axis=0, concat_axis=0, tiled=True)

    block = 8
    out = (pairs, rows, cols)
    return pl.pallas_call(
        functools.partial(finish_kernel, rows=rows, cols=cols, pairs=pairs, block=block),
        in_specs=[smem(), *[vmem()] * 6],
        out_specs=[hbm()] * 2,
        out_shape=[shaped(out)] * 2,
        scratch_shapes=[
            pltpu.VMEM((pairs, TILE), f32),
            pltpu.VMEM((pairs, TILE), f32),
            pltpu.VMEM(out, f32),
            pltpu.VMEM(out, f32),
            pltpu.SemaphoreType.DMA((pairs // block,)),
            pltpu.SemaphoreType.DMA((pairs // block,)),
        ],
        compiler_params=limit,
        name="finish",
    )(index, everyone, field, pre, image, second, last)


def solution(mesh):
    cells = P(("groups", "space"), None)
    return jax.shard_map(
        on_device,
        mesh=mesh,
        in_specs=(*[cells] * 6, P(("groups", "space"), None, None, None), P(("groups", "rhs"), None)),
        out_specs=(P("rhs", ("groups", "space"), None), P("rhs", ("groups", "space"), None)),
        check_vma=False,
    )
```
